128 devices in a mesh: tm: 128 (over x, z, y, core).
Axes of the slice: x: 4, y: 4, z: 4, core: 2. Of those that a mesh axis runs over, the one named last changes fastest.
Arguments:
- field: bfloat16 [43008, 8192], P('tm'), may hold values from -52 to 52
- index: float32 [43008, 10], P('tm'), may hold values from -13 to 13
- lag_list: int32 [61], replicated, may hold values from -30 to 30, as said below
- index_offset: int32 [10], replicated, may hold values from 0 to 14, as said below
- sea_mask: int32 [8192], P('tm'), may hold values 0 or 1
Outputs:
- corr_maps: float32 [8192, 10, 61], P('tm')
The draws below stay inside these ranges and needn't reach their ends.
Inputs may be any that keep to these rules, and one draw needn't show every extreme that they name: `lag_list`: each whole number of -30 to 30 appears once. `index_offset`: some index has the extra lead 14.
All inputs are finite; a program needn't handle non-finite values. No bound on the sum of `sea_mask` on one device may be relied on, other than what follows from the above.
Results may differ from the reference program's by a relative error of at most 0.00051.
Values may be sent and summed in bfloat16 or wider, within the bound.
No kernel may reach another device: no remote copies, remote signals or barrier semaphores. Data moves between devices by JAX's collectives and lax.ppermute only.
A program may use at most 256 MiB of HBM per device.

```python
import jax
import jax.numpy as jnp
from jax import lax

T_DEV = 336
INDEX_COUNT = 10
MAXLAG = 30
MAXOFF = 14
LAGS = 61
TDAYS = 43008
CELLS = 8192
N_TM = 128


def index_base(key):
    keys = jax.random.split(jax.random.fold_in(key, 11), 2)
    times = jnp.arange(TDAYS, dtype=jnp.float32)[:, None]
    envelope = 1.0 + 2.0 * times / (TDAYS - 1.0)
    noise = jax.random.truncated_normal(keys[0], -4.0, 4.0, (TDAYS, INDEX_COUNT), jnp.float32)
    offset_means = jax.random.uniform(keys[1], (INDEX_COUNT,), jnp.float32, -0.5, 0.5)
    return envelope * noise + offset_means[None, :]


def draw_index(key, part):
    return index_base(key)


def draw_field(key, part):
    series = index_base(key)
    keys = jax.random.split(jax.random.fold_in(key, 23), 6)
    linked = jax.random.randint(keys[0], (CELLS,), 0, INDEX_COUNT)
    delays = jax.random.randint(keys[1], (CELLS,), -MAXLAG, MAXLAG + MAXOFF + 1)
    weights = jax.random.uniform(keys[2], (CELLS,), jnp.float32, 0.3, 1.0) * jnp.where(jax.random.randint(keys[3], (CELLS,), 0, 2) == 0, -1.0, 1.0)
    scales = jnp.exp(jax.random.uniform(keys[4], (CELLS,), jnp.float32, jnp.log(0.3), jnp.log(3.0)))
    times = jnp.arange(TDAYS, dtype=jnp.int32)[:, None]
    source = jnp.clip(times - delays[None, :], 0, TDAYS - 1)
    signal = series[source, linked[None, :]]
    noise = jax.random.truncated_normal(keys[5], -4.0, 4.0, (TDAYS, CELLS), jnp.float32)
    cell_means = 0.5 * weights
    return (scales[None, :] * (weights[None, :] * signal + noise + cell_means[None, :])).astype(jnp.bfloat16)


def draw_lag_list(key, part):
    order = jax.random.permutation(jax.random.fold_in(key, 31), LAGS)
    return (order - MAXLAG).astype(jnp.int32)


def draw_index_offset(key, part):
    keys = jax.random.split(jax.random.fold_in(key, 37), 2)
    series_values = jax.random.randint(keys[0], (INDEX_COUNT,), 0, MAXOFF + 1)
    chosen = jax.random.randint(keys[1], (), 0, INDEX_COUNT)
    return series_values.at[chosen].set(MAXOFF).astype(jnp.int32)


def place_ends(drawn, stream_key, smallest, high):
    dims = drawn.shape
    index_at = [jax.random.randint(jax.random.fold_in(stream_key, axis), (), 0, dims[axis]) for axis in range(len(dims))]
    drawn = drawn.at[tuple(index_at)].set(smallest)
    longest = dims.index(max(dims))
    index_at[longest] = (index_at[longest] + 1) % dims[longest]
    return drawn.at[tuple(index_at)].set(high)


def setup_inputs(seed: int = 0) -> dict:
    streams_of = jax.random.split(jax.random.key(seed), 6)
    field = draw_field(jax.random.fold_in(streams_of[5], 71), 0)
    index = draw_index(jax.random.fold_in(streams_of[5], 71), 0)
    lag_list = draw_lag_list(jax.random.fold_in(streams_of[5], 71), 0)
    index_offset = draw_index_offset(jax.random.fold_in(streams_of[5], 71), 0)
    sea_mask = place_ends((jax.random.randint(streams_of[4], (CELLS,), 0, 10) < 7).astype(jnp.int32), jax.random.fold_in(streams_of[4], 1), 0, 1)
    return dict(field=field, index=index, lag_list=lag_list, index_offset=index_offset, sea_mask=sea_mask)


def build_window_sums(padded, begin, length, reach, lag_low):
    count = reach + lag_low + 1
    piece = lax.dynamic_slice_in_dim(padded, begin, length + reach + lag_low, 0)
    windows = jnp.stack([piece[reach + lag_low - j:reach + lag_low - j + length] for j in range(count)], 1)
    return windows.reshape(length, count * padded.shape[1])

def lag_selector(shifts, reach, lag_low):
    count = reach + lag_low + 1
    places = jnp.arange(count, dtype=jnp.int32)
    return (places[None, :, None] == (shifts + lag_low)[:, None, :]).astype(jnp.float32)

def pick_lags(accum, selector):
    kcount, count, lcount = selector.shape
    spread = accum.reshape(accum.shape[0], count, kcount)
    chosen = jnp.einsum('cjk,kjl->ckl', spread, selector, precision=lax.Precision.HIGHEST)
    return chosen.reshape(accum.shape[0], kcount * lcount)

def reference(field, index, lag_list, index_offset, sea_mask):
    reach = MAXLAG + MAXOFF
    count = reach + MAXLAG + 1
    total_days = TDAYS * 1.0
    mean_i = lax.optimization_barrier(jnp.sum(index, 0)) / total_days
    var_i = lax.optimization_barrier(jnp.sum(index * index, 0)) / total_days - mean_i * mean_i
    centered = (index - mean_i).astype(jnp.bfloat16)
    shifts = (lag_list[None, :] + index_offset[:, None]).astype(jnp.int32)
    padded = jnp.pad(centered, ((reach, reach), (0, 0)))
    running_total = jnp.concatenate([jnp.zeros((1, INDEX_COUNT), jnp.float32), jnp.cumsum(padded.astype(jnp.float32), 0)], 0)
    upper_bound = (TDAYS - shifts + reach).astype(jnp.int32)
    lower_bound = (reach - shifts).astype(jnp.int32)
    series_number = jnp.arange(INDEX_COUNT, dtype=jnp.int32)[:, None]
    prefix_totals = running_total[upper_bound, series_number] - running_total[lower_bound, series_number]
    selector = lag_selector(shifts, reach, MAXLAG)
    block_rows = 8 * T_DEV
    turns = N_TM // 8

    def one_block(carry, turn):
        accum, first_sum, second_sum = carry
        begin = (turn * block_rows).astype(jnp.int32)
        rows = lax.dynamic_slice_in_dim(field, begin, block_rows, 0)
        windows = build_window_sums(padded, begin, block_rows, reach, MAXLAG)
        accum = accum + lax.dot_general(rows, windows, (((0,), (0,)), ((), ())), preferred_element_type=jnp.float32)
        wide = rows.astype(jnp.float32)
        return ((accum, first_sum + lax.optimization_barrier(jnp.sum(wide, 0)), second_sum + lax.optimization_barrier(jnp.sum(wide * wide, 0))), None)
    start_carry = (jnp.zeros((CELLS, count * INDEX_COUNT), jnp.float32), jnp.zeros((CELLS,), jnp.float32), jnp.zeros((CELLS,), jnp.float32))
    (accum, first_sum, second_sum), unused = lax.scan(one_block, start_carry, jnp.arange(turns, dtype=jnp.int32))
    products = pick_lags(accum, selector)
    mean_x = first_sum / total_days
    var_x = second_sum / total_days - mean_x * mean_x
    numer = products.reshape(CELLS, INDEX_COUNT, LAGS) - mean_x[:, None, None] * prefix_totals[None]
    scale = total_days * jnp.sqrt(var_x + 1e-06)[:, None, None] * jnp.sqrt(var_i + 1e-06)[None, :, None]
    return numer / scale * sea_mask.astype(jnp.float32)[:, None, None]
```

```python
import functools

import jax
import jax.numpy as jnp
from jax import lax
from jax.experimental import pallas as pl
from jax.experimental.pallas import tpu as pltpu
from jax.sharding import Mesh
from jax.sharding import PartitionSpec as P

MAXLAG = 30
MAXOFF = 14
CHIPS = ("tm_0", "tm_1", "tm_2")
CORE = "tm_3"
TM = CHIPS + (CORE,)
PHASES = 6
LANES = 128
HALF = 64


def pack_kernel(field_ref, index_ref, order_ref, out_ref, index_rows):
    t_dev, kcount = index_ref.shape
    count = t_dev // PHASES
    order = order_ref[...]

    @pl.when(pl.program_id(0) == 0)
    def _():
        value = index_ref[...]
        upper = value.astype(jnp.bfloat16)
        lower = (value - upper.astype(jnp.float32)).astype(jnp.bfloat16)
        rows = []
        for part in (upper, lower):
            sorted_part = jnp.dot(order, part, preferred_element_type=jnp.float32)
            rows.extend(sorted_part[r * count : (r + 1) * count] for r in range(PHASES))
            rows.append(jnp.zeros((count, HALF - PHASES * kcount), jnp.float32))
        index_rows[...] = jnp.concatenate(rows, axis=1).astype(jnp.bfloat16)

    for chip in range(out_ref.shape[0]):
        block = field_ref[:, chip * LANES : (chip + 1) * LANES]
        sorted_block = jnp.dot(order, block, preferred_element_type=jnp.float32)
        out_ref[chip, 0:t_dev, :] = sorted_block.astype(jnp.bfloat16)
        out_ref[chip, t_dev:, :] = index_rows[...]


def pack(field, index):
    t_dev, cells = field.shape
    chips = cells // LANES
    count = t_dev // PHASES
    step = 8
    row = jnp.arange(t_dev)
    day = (row % count) * PHASES + row // count
    order = (day[:, None] == jnp.arange(t_dev)[None, :]).astype(jnp.bfloat16)
    return pl.pallas_call(
        pack_kernel,
        grid=(chips // step,),
        in_specs=[
            pl.BlockSpec((t_dev, step * LANES), lambda i: (0, i)),
            pl.BlockSpec(index.shape, lambda i: (0, 0)),
            pl.BlockSpec((t_dev, t_dev), lambda i: (0, 0)),
        ],
        out_specs=pl.BlockSpec((step, t_dev + count, LANES), lambda i: (i, 0, 0)),
        out_shape=jax.ShapeDtypeStruct((chips, t_dev + count, LANES), jnp.bfloat16),
        scratch_shapes=[pltpu.VMEM((count, LANES), jnp.bfloat16)],
    )(field, index, order)


def shards(field, index, lag_list, index_offset, sea_mask):
    t_dev, kcount = index.shape
    count = t_dev // PHASES
    chips = field.shape[1] // LANES
    total_days = t_dev * lax.axis_size(TM) * 1.0
    core = lax.axis_index(CORE)
    swap = [(0, 1), (1, 0)]
    used = PHASES * kcount

    sent = pack(field, index)
    got = lax.all_to_all(sent, CHIPS, 0, 0, tiled=True)
    days = got[:, :t_dev].reshape(chips, PHASES, count, LANES)
    own_raw = got[:, t_dev:]
    other_raw = lax.ppermute(own_raw, CORE, swap)

    def joined(raw):
        return (raw[..., :HALF].astype(jnp.float32) + raw[..., HALF:].astype(jnp.float32))[..., :used]

    own, other = joined(own_raw), joined(other_raw)
    first = (jnp.sum(own, (0, 1)) + jnp.sum(other, (0, 1))).reshape(PHASES, kcount).sum(0)
    second = (jnp.sum(own * own, (0, 1)) + jnp.sum(other * other, (0, 1))).reshape(PHASES, kcount).sum(0)
    mean_i = first / total_days
    var_i = second / total_days - mean_i * mean_i
    mean_row = jnp.tile(mean_i, PHASES)
    own = (own - mean_row).astype(jnp.bfloat16)
    other = (other - mean_row).astype(jnp.bfloat16)
    edge = jnp.pad(other, ((1, 1), (0, 0), (0, 0)))
    before = lax.dynamic_slice_in_dim(edge, core, chips, 0)[:, count - 8 :]
    after = lax.dynamic_slice_in_dim(edge, core + 1, chips, 0)[:, :8]
    extended = jnp.concatenate([before, own, after], 1)
    windows = jnp.concatenate([extended[:, m : m + count] for m in range(14)], 2)
    spread = jnp.einsum("irbc,ibw->rcw", days, windows, preferred_element_type=jnp.float32)
    spread = spread.reshape(PHASES, LANES, 14 * PHASES, kcount)
    window_sums = jnp.sum(windows.astype(jnp.float32), (0, 1)).reshape(14 * PHASES, kcount)
    lags_all = MAXLAG + MAXLAG + MAXOFF + 1
    accum = sum(spread[r, :, 4 + r : 4 + r + lags_all] for r in range(PHASES))
    totals = sum(window_sums[4 + r : 4 + r + lags_all] for r in range(PHASES))
    wide = days.astype(jnp.float32)
    first_sum = jnp.sum(wide, (0, 1, 2))
    second_sum = jnp.sum(wide * wide, (0, 1, 2))

    def swapped(mine):
        halves = mine.reshape(2, HALF, *mine.shape[1:])
        kept = lax.dynamic_index_in_dim(halves, core, 0, keepdims=False)
        passed = lax.dynamic_index_in_dim(halves, 1 - core, 0, keepdims=False)
        return kept + lax.ppermute(passed, CORE, swap)

    accum = swapped(accum)
    sums = swapped(jnp.stack([first_sum, second_sum], 1))
    totals = totals + lax.ppermute(totals, CORE, swap)
    shifts = lag_list[None, :] + index_offset[:, None]
    place = MAXLAG + MAXOFF - shifts
    selector = (jnp.arange(lags_all)[None, :, None] == place[:, None, :]).astype(jnp.float32)
    products = jnp.einsum("cjk,kjl->ckl", accum, selector, precision=lax.Precision.HIGHEST)
    prefix_totals = jnp.einsum("jk,kjl->kl", totals, selector, precision=lax.Precision.HIGHEST)
    mean_x = sums[:, 0] / total_days
    var_x = sums[:, 1] / total_days - mean_x * mean_x
    numer = products - mean_x[:, None, None] * prefix_totals[None]
    scale = (
        total_days * jnp.sqrt(var_x + 1e-06)[:, None, None] * jnp.sqrt(var_i + 1e-06)[None, :, None]
    )
    return numer / scale * sea_mask.astype(jnp.float32)[:, None, None]


def solution(mesh):
    finer = Mesh(mesh.devices.reshape(4, 4, 4, 2), TM)
    return jax.shard_map(
        shards,
        mesh=finer,
        in_specs=(P(TM, None), P(TM, None), P(), P(), P(TM)),
        out_specs=P(TM, None, None),
        check_vma=False,
    )
```

```python
import jax
import jax.numpy as jnp
from jax import lax
from jax.experimental import pallas as pl
from jax.experimental.pallas import tpu as pltpu
from jax.sharding import Mesh
from jax.sharding import PartitionSpec as P

MAXLAG = 30
MAXOFF = 14
CHIPS = ("tm_0", "tm_1", "tm_2")
CORE = "tm_3"
TM = CHIPS + (CORE,)
PHASES = 6
LANES = 128
HALF = 64
BEFORE = 8
TILES = 7
WIDTH = TILES * LANES
SUM_LANE = BEFORE * HALF + 60
SQUARE_LANE = SUM_LANE + 1
ROWS = HALF + 8
F32 = jnp.float32
BF16 = jnp.bfloat16


def pack_kernel(field_ref, index_ref, order_ref, out_ref, index_rows):
    t_dev, kcount = index_ref.shape
    count = t_dev // PHASES
    order = order_ref[...]

    @pl.when(pl.program_id(0) == 0)
    def _():
        value = index_ref[...]
        upper = value.astype(BF16)
        lower = (value - upper.astype(F32)).astype(BF16)
        rows = []
        for part in (upper, lower):
            sorted_part = jnp.dot(order, part, preferred_element_type=F32)
            rows.extend(sorted_part[r * count : (r + 1) * count] for r in range(PHASES))
            rows.append(jnp.zeros((count, HALF - PHASES * kcount), F32))
        index_rows[...] = jnp.concatenate(rows, axis=1).astype(BF16)

    for pair in range(out_ref.shape[0] // 2):
        block = field_ref[:, pair * 2 * LANES : (pair + 1) * 2 * LANES]
        sorted_block = jnp.dot(order, block, preferred_element_type=F32).astype(BF16)
        out_ref[2 * pair, 0:t_dev, :] = sorted_block[:, :LANES]
        out_ref[2 * pair + 1, 0:t_dev, :] = sorted_block[:, LANES:]
        out_ref[2 * pair, t_dev:, :] = index_rows[...]
        out_ref[2 * pair + 1, t_dev:, :] = index_rows[...]


def pack(field, index):
    t_dev, cells = field.shape
    chips = cells // LANES
    count = t_dev // PHASES
    step = 8
    row = jnp.arange(t_dev)
    day = (row % count) * PHASES + row // count
    order = (day[:, None] == jnp.arange(t_dev)[None, :]).astype(BF16)
    return pl.pallas_call(
        pack_kernel,
        grid=(chips // step,),
        in_specs=[
            pl.BlockSpec((t_dev, step * LANES), lambda i: (0, i)),
            pl.BlockSpec(index.shape, lambda i: (0, 0)),
            pl.BlockSpec((t_dev, t_dev), lambda i: (0, 0)),
        ],
        out_specs=pl.BlockSpec((step, t_dev + count, LANES), lambda i: (i, 0, 0)),
        out_shape=jax.ShapeDtypeStruct((chips, t_dev + count, LANES), BF16),
        scratch_shapes=[pltpu.VMEM((count, LANES), BF16)],
    )(field, index, order)


def square_kernel(got_ref, out_ref):
    @pl.when(pl.program_id(0) == 0)
    def _():
        out_ref[...] = jnp.zeros_like(out_ref)

    wide = got_ref[...].astype(F32)
    groups = (wide * wide).reshape(-1, 8, LANES)
    out_ref[...] += jnp.sum(groups, 0)


def squares(got, t_dev):
    chips = got.shape[0]
    step = 8
    return pl.pallas_call(
        square_kernel,
        grid=(chips // step,),
        in_specs=[pl.BlockSpec((step, t_dev, LANES), lambda i: (i, 0, 0))],
        out_specs=pl.BlockSpec((8, LANES), lambda i: (0, 0)),
        out_shape=jax.ShapeDtypeStruct((8, LANES), F32),
    )(got)


def joined(raw):
    wide = raw.astype(F32)
    return wide + pltpu.roll(wide, HALF, 2)


def shifted(parts):
    total = parts[0]
    lane = lax.broadcasted_iota(jnp.int32, total.shape, 1) % HALF
    for r in range(1, PHASES):
        near = pltpu.roll(parts[r], WIDTH - 10 * r, 1)
        far = pltpu.roll(parts[r], WIDTH - 10 * r - 4, 1)
        total = total + jnp.where(lane + 10 * r < 60, near, far)
    return total


def spread_kernel(
    core_ref, own_ref, other_ref, square_ref, got_ref,
    kept_ref, passed_ref, stat_ref,
    days, edge, ext, win, acc, sems,
):
    chips, count, _ = own_ref.shape
    core = core_ref[0]
    copies = []
    for r in range(PHASES):
        copy = pltpu.make_async_copy(
            got_ref.at[:, r * count : (r + 1) * count, :], days.at[r], sems.at[r]
        )
        copy.start()
        copies.append(copy)

    total_days = 2.0 * chips * count * PHASES
    own = joined(own_ref[...])
    other = joined(other_ref[...])
    first = jnp.sum(own, (0, 1), keepdims=True)[0] + jnp.sum(other, (0, 1), keepdims=True)[0]
    second = (
        jnp.sum(own * own, (0, 1), keepdims=True)[0]
        + jnp.sum(other * other, (0, 1), keepdims=True)[0]
    )
    row = lax.broadcasted_iota(jnp.int32, (LANES, LANES), 0)
    column = lax.broadcasted_iota(jnp.int32, (LANES, LANES), 1) % HALF
    same = (row < 60) & (column < 60) & (row % 10 == column % 10)
    sums = jnp.concatenate([first, second, jnp.zeros((6, LANES), F32)], 0)
    folded = jnp.dot(
        sums, same.astype(F32), precision=lax.Precision.HIGHEST, preferred_element_type=F32
    )
    mean = folded[0:1] / total_days
    var = folded[1:2] / total_days - mean * mean
    stat_ref[...] = jnp.concatenate([mean, var, jnp.zeros((6, LANES), F32)], 0)
    lane = lax.broadcasted_iota(jnp.int32, (1, 1, LANES), 2)
    valid = lane % HALF < 60

    def centered(value):
        return jnp.where(valid, (value - mean[None]).astype(BF16).astype(F32), 0.0)

    own = centered(own)
    other = centered(other)
    zero = jnp.zeros((1, 16, LANES), F32)
    edge[0:1] = zero
    edge[chips + 1 : chips + 2] = zero
    edge[1 : chips + 1, 0:8, :] = other[:, 0:8, :]
    edge[1 : chips + 1, 8:16, :] = other[:, count - 8 :, :]
    ext[:, 0:8, :] = edge[pl.ds(core, chips), 8:16, :]
    ext[:, 8 : 8 + count, :] = jnp.where(lane == 60, 1.0, own)
    ext[:, 8 + count :, :] = edge[pl.ds(core + 1, chips), 0:8, :]
    window_sums = []
    for q in range(TILES):
        tile = jnp.where(
            lane < HALF,
            ext[:, 2 * q : 2 * q + count, :],
            ext[:, 2 * q + 1 : 2 * q + 1 + count, :],
        )
        window_sums.append(jnp.sum(tile, (0, 1), keepdims=True)[0])
        tile = tile.astype(BF16)
        for chip in range(chips):
            win[chip * count : (chip + 1) * count, q * LANES : (q + 1) * LANES] = tile[chip]
    for copy in copies:
        copy.wait()
    for r in range(PHASES):
        flat = days.at[r].reshape(chips * count, LANES)[...]
        acc[r * LANES : (r + 1) * LANES, :] = lax.dot_general(
            flat, win[...], (((0,), (0,)), ((), ())), preferred_element_type=F32
        )
    parts = [acc[r * LANES : (r + 1) * LANES, :] for r in range(PHASES)]
    result = shifted(parts)
    plain = sum(parts)
    squared = jnp.sum(square_ref[...], 0, keepdims=True)
    square_column = jnp.transpose(jnp.broadcast_to(squared, (LANES, LANES)))[:, 0:1]
    lanes = lax.broadcasted_iota(jnp.int32, result.shape, 1)
    result = jnp.where(lanes == SUM_LANE, plain, result)
    result = jnp.where(lanes == SQUARE_LANE, square_column, result)
    acc[0:LANES, :] = result
    sums_row = jnp.broadcast_to(jnp.concatenate(window_sums, 1), (8, WIDTH))
    totals = shifted([sums_row] * PHASES)
    kept_ref[0:HALF, :] = acc[pl.ds(pl.multiple_of(core * HALF, HALF), HALF), :]
    passed_ref[0:HALF, :] = acc[pl.ds(pl.multiple_of((1 - core) * HALF, HALF), HALF), :]
    kept_ref[HALF:, :] = totals
    passed_ref[HALF:, :] = totals


def spread(core, own, other, square, got):
    chips, count, _ = own.shape
    vmem = pl.BlockSpec(memory_space=pltpu.VMEM)
    half = jax.ShapeDtypeStruct((ROWS, WIDTH), F32)
    return pl.pallas_call(
        spread_kernel,
        in_specs=[pl.BlockSpec(memory_space=pltpu.SMEM), vmem, vmem, vmem, pl.BlockSpec(memory_space=pl.ANY)],
        out_specs=[vmem] * 3,
        out_shape=[half, half, jax.ShapeDtypeStruct((8, LANES), F32)],
        scratch_shapes=[
            pltpu.VMEM((PHASES, chips, count, LANES), BF16),
            pltpu.VMEM((chips + 2, 16, LANES), F32),
            pltpu.VMEM((chips, count + 16, LANES), F32),
            pltpu.VMEM((chips * count, WIDTH), BF16),
            pltpu.VMEM((PHASES * LANES, WIDTH), F32),
            pltpu.SemaphoreType.DMA((PHASES,)),
        ],
        compiler_params=pltpu.CompilerParams(vmem_limit_bytes=60 << 20),
    )(core, own, other, square, got)


def finish_kernel(kept_ref, taken_ref, stat_ref, place_ref, mask_ref, days_ref, out_ref):
    total_days = days_ref[0]
    value = kept_ref[...] + taken_ref[...]
    upper = value.astype(BF16)
    rest = value - upper.astype(F32)
    middle = rest.astype(BF16)
    lower = (rest - middle.astype(F32)).astype(BF16)
    mean_x = value[0:HALF, SUM_LANE : SUM_LANE + 1] / total_days
    var_x = value[0:HALF, SQUARE_LANE : SQUARE_LANE + 1] / total_days - mean_x * mean_x
    scale_x = total_days * jnp.sqrt(var_x + 1e-06)
    scale_i = jnp.sqrt(stat_ref[1:2, :] + 1e-06)
    mask = mask_ref[...].astype(F32)
    row = lax.broadcasted_iota(jnp.int32, (WIDTH, LANES), 0)
    for k in range(out_ref.shape[1]):
        selector = (row == place_ref[k : k + 1, :]).astype(BF16)
        chosen = (
            jnp.dot(upper, selector, preferred_element_type=F32)
            + jnp.dot(middle, selector, preferred_element_type=F32)
            + jnp.dot(lower, selector, preferred_element_type=F32)
        )
        numer = chosen[0:HALF] - mean_x * chosen[HALF : HALF + 1]
        answer = numer / (scale_x * scale_i[:, k : k + 1]) * mask
        out_ref[:, k, :] = answer[:, : out_ref.shape[2]]


def finish(kept, taken, stat, place, mask, total_days, lags):
    vmem = pl.BlockSpec(memory_space=pltpu.VMEM)
    kcount = place.shape[0]
    return pl.pallas_call(
        finish_kernel,
        in_specs=[vmem] * 5 + [pl.BlockSpec(memory_space=pltpu.SMEM)],
        out_specs=vmem,
        out_shape=jax.ShapeDtypeStruct((HALF, kcount, lags), F32),
    )(kept, taken, stat, place, mask, total_days)


def shards(field, index, lag_list, index_offset, sea_mask):
    t_dev, kcount = index.shape
    swap = [(0, 1), (1, 0)]
    total_days = jnp.full((1,), t_dev * lax.axis_size(TM), F32)
    core = lax.axis_index(CORE).astype(jnp.int32).reshape(1)
    got = lax.all_to_all(pack(field, index), CHIPS, 0, 0, tiled=True)
    own = got[:, t_dev:]
    other = lax.ppermute(own, CORE, swap)
    square = squares(got, t_dev)
    kept, passed, stat = spread(core, own, other, square, got)
    taken = lax.ppermute(passed, CORE, swap)
    shifts = lag_list[None, :] + index_offset[:, None]
    slot = BEFORE * PHASES - shifts
    place = HALF * (slot // PHASES) + kcount * (slot % PHASES) + jnp.arange(kcount)[:, None]
    place = jnp.pad(place, ((0, 0), (0, LANES - place.shape[1])), constant_values=-1)
    return finish(
        kept, taken, stat, place.astype(jnp.int32), sea_mask[:, None], total_days, lag_list.shape[0]
    )


def solution(mesh):
    finer = Mesh(mesh.devices.reshape(4, 4, 4, 2), TM)
    return jax.shard_map(
        shards,
        mesh=finer,
        in_specs=(P(TM, None), P(TM, None), P(), P(), P(TM)),
        out_specs=P(TM, None, None),
        check_vma=False,
    )
```

```python
import jax
import jax.numpy as jnp
from jax import lax
from jax.experimental import pallas as pl
from jax.experimental.pallas import tpu as pltpu
from jax.sharding import PartitionSpec as P

TM = "tm"
CORES = 2
WEIGHTS = (1, 16, 4)
DIGITS = ((3, 2, 1, 0), (3, 2, 1, 0), (2, 3, 0, 1))
PHASES = 6
KCOUNT = 10
USED = PHASES * KCOUNT
LANES = 128
HALF = 64
BEFORE = 8
TILES = 7
WIDTH = TILES * LANES
SUM_LANE = BEFORE * HALF + USED
SQUARE_LANE = SUM_LANE + 1
ROWS = HALF + 16
STEP = 8
EARLY = 32
F32 = jnp.float32
BF16 = jnp.bfloat16
VMEM = pl.BlockSpec(memory_space=pltpu.VMEM)
ANY = pl.BlockSpec(memory_space=pl.ANY)
SMALL = pltpu.CompilerParams(vmem_limit_bytes=8 << 20)


def chip_at(place):
    chip = 0
    for i, (weight, digits) in enumerate(zip(WEIGHTS, DIGITS)):
        digit = (place >> (4 - 2 * i)) & 3
        table = sum(value << (2 * at) for at, value in enumerate(digits))
        chip = chip + weight * ((table >> (2 * digit)) & 3)
    return chip


def local(array):
    return pltpu.with_memory_space_constraint(array, pltpu.VMEM)


def fill_order(early, late):
    for target in (early, late):
        days = target.shape[0]
        length = days // PHASES
        row = lax.broadcasted_iota(jnp.int32, (length, days), 0)
        column = lax.broadcasted_iota(jnp.int32, (length, days), 1)
        for r in range(PHASES):
            target[r * length : (r + 1) * length, :] = (column == row * PHASES + r).astype(BF16)


def order_scratch(t_dev):
    ahead = EARLY * PHASES
    return [pltpu.VMEM((ahead, ahead), BF16), pltpu.VMEM((t_dev - ahead, t_dev - ahead), BF16)]


def pack_kernel(field_ref, index_ref, sent_ref, index, early, late, sems, index_sem):
    kcount, t_dev = index_ref.shape
    count = t_dev // PHASES
    chips = sent_ref.shape[0]
    ahead = EARLY * PHASES
    index_copy = pltpu.make_async_copy(index_ref, index, index_sem)
    index_copy.start()

    def copy(place):
        lanes = pl.ds(pl.multiple_of(chip_at(place) * LANES, LANES), LANES)
        return pltpu.make_async_copy(
            field_ref.at[:, lanes], sent_ref.at[place, 0:t_dev, :], sems.at[place]
        )

    def start(place, _):
        copy(place).start()
        return 0

    lax.fori_loop(0, chips, start, 0, unroll=8)
    fill_order(early, late)
    index_copy.wait()
    value = index[...]
    upper = value.astype(BF16)
    lower = (value - upper.astype(F32)).astype(BF16)
    pieces = []
    for part in (upper, lower):
        first = lax.dot_general(
            early[...], part[:, :ahead], (((1,), (1,)), ((), ())), preferred_element_type=F32
        )
        second = lax.dot_general(
            late[...], part[:, ahead:], (((1,), (1,)), ((), ())), preferred_element_type=F32
        )
        for r in range(PHASES):
            pieces.append(
                jnp.concatenate(
                    [
                        first[r * EARLY : (r + 1) * EARLY],
                        second[r * (count - EARLY) : (r + 1) * (count - EARLY)],
                    ],
                    0,
                )
            )
        pieces.append(jnp.zeros((count, HALF - USED), F32))
    rows = jnp.concatenate(pieces, axis=1).astype(BF16)

    def repeat(place, _):
        sent_ref[place, t_dev:, :] = rows
        return 0

    lax.fori_loop(0, chips, repeat, 0, unroll=8)

    def finish_copy(place, _):
        copy(place).wait()
        return 0

    lax.fori_loop(0, chips, finish_copy, 0, unroll=8)


def pack(field, index):
    t_dev, cells = field.shape
    chips = cells // LANES
    return pl.pallas_call(
        pack_kernel,
        in_specs=[ANY] * 2,
        out_specs=VMEM,
        out_shape=pltpu.VMEM((chips, t_dev + t_dev // PHASES, LANES), BF16),
        scratch_shapes=[pltpu.VMEM(index.T.shape, F32)]
        + order_scratch(t_dev)
        + [pltpu.SemaphoreType.DMA((chips,)), pltpu.SemaphoreType.DMA],
        compiler_params=SMALL,
    )(*[pltpu.with_memory_space_constraint(x, pltpu.HBM) for x in (field, index.T)])


def joined(raw):
    wide = raw.astype(F32)
    return wide + pltpu.roll(wide, HALF, 1)


def summed(value):
    return jnp.sum(value.reshape(-1, 8, LANES), 0)


def take_kernel(got_ref, own_ref, edge_ref):
    chips, count, _ = own_ref.shape
    zero = jnp.zeros((8, LANES), F32)

    def body(place, sums):
        first, second = sums
        chip = chip_at(place)
        value = joined(got_ref[place, PHASES * count :, :])
        own_ref[place] = value
        edge_ref[chip, 0:8, :] = value[0:8]
        edge_ref[chip, 8:16, :] = value[count - 8 :]
        return first + summed(value), second + summed(value * value)

    first, second = lax.fori_loop(0, chips, body, (zero, zero), unroll=16)
    edge_ref[chips, 0:8, :] = first
    edge_ref[chips, 8:16, :] = second


def take_index(got, count):
    chips = got.shape[0]
    return pl.pallas_call(
        take_kernel,
        in_specs=[VMEM],
        out_specs=[VMEM] * 2,
        out_shape=[
            pltpu.VMEM((chips, count, LANES), F32),
            pltpu.VMEM((chips + 1, 16, LANES), F32),
        ],
        compiler_params=SMALL,
    )(local(got))


def middle_kernel(got_ref, days_ref, square_ref, early, late):
    chips, rows, _ = got_ref.shape
    t_dev = rows * PHASES // (PHASES + 1)
    count = t_dev // PHASES
    ahead = EARLY * PHASES
    fill_order(early, late)

    def body(pair, square):
        start = pl.multiple_of(pair * 2 * count, 16)
        for source, days, base in ((early, slice(0, ahead), 0), (late, slice(ahead, t_dev), EARLY)):
            length = source.shape[0] // PHASES
            blocks = [got_ref[2 * pair + side, days, :] for side in range(2)]
            for block in blocks:
                wide = block.astype(F32)
                square = square + jnp.sum((wide * wide).reshape(-1, 16, LANES), 0)
            mixed = jnp.dot(
                source[...], jnp.concatenate(blocks, 1), preferred_element_type=F32
            )
            for r in range(PHASES):
                piece = mixed[r * length : (r + 1) * length].astype(BF16)
                days_ref[r, pl.ds(start + base, length), :] = piece[:, :LANES]
                days_ref[r, pl.ds(start + count + base, length), :] = piece[:, LANES:]
        return square

    square_ref[...] = lax.fori_loop(0, chips // 2, body, jnp.zeros((16, LANES), F32), unroll=8)


def middle(got, t_dev):
    chips = got.shape[0]
    return pl.pallas_call(
        middle_kernel,
        in_specs=[VMEM],
        out_specs=[VMEM] * 2,
        out_shape=[
            pltpu.VMEM((PHASES, chips * t_dev // PHASES, LANES), BF16),
            pltpu.VMEM((16, LANES), F32),
        ],
        scratch_shapes=order_scratch(t_dev),
        compiler_params=SMALL,
    )(local(got))


def spread_kernel(
    own, mine_ref, other_ref, square_ref, days,
    kept_ref, passed_ref, stat_ref,
    edge, line, slid, win, acc, merged,
):
    chips, count, _ = own.shape
    core = lax.rem(lax.axis_index(TM), CORES)
    total_days = 2.0 * chips * count * PHASES
    zero = jnp.zeros((8, LANES), F32)
    sums = mine_ref[chips] + other_ref[chips]
    row = lax.broadcasted_iota(jnp.int32, (LANES, LANES), 0)
    column = lax.broadcasted_iota(jnp.int32, (LANES, LANES), 1) % HALF
    same = (row < USED) & (column < USED) & (row % KCOUNT == column % KCOUNT)
    folded = jnp.dot(
        sums, same.astype(F32), precision=lax.Precision.HIGHEST, preferred_element_type=F32
    )
    mean = jnp.sum(folded[0:8], 0, keepdims=True) / total_days
    var = jnp.sum(folded[8:16], 0, keepdims=True) / total_days - mean * mean
    stat_ref[...] = jnp.concatenate([mean, var, jnp.zeros((6, LANES), F32)], 0)
    lane = lax.broadcasted_iota(jnp.int32, (1, LANES), 1)
    valid = lane % HALF < USED

    def centered(value):
        return jnp.where(valid, (value - mean).astype(BF16).astype(F32), 0.0)

    edge[0] = jnp.broadcast_to(mean, (16, LANES))
    edge[chips + 1] = jnp.broadcast_to(mean, (16, LANES))

    def move(chip, _):
        edge[chip + 1] = other_ref[chip]
        return 0

    lax.fori_loop(0, chips, move, 0, unroll=16)

    def slide(group, sums):
        sums = list(sums)
        for side in range(8):
            place = 8 * group + side
            chip = chip_at(place)
            line[side, 0:8, :] = centered(edge[chip + core, 8:16, :])
            line[side, 8 : 8 + count, :] = jnp.where(lane == USED, 1.0, centered(own[place]))
            line[side, 8 + count :, :] = centered(edge[chip + core + 1, 0:8, :])
        for side in range(8):
            slid[side, 0 : count + 15, :] = jnp.where(
                lane < HALF, line[side, 0 : count + 15, :], line[side, 1 : count + 16, :]
            )
        start = pl.multiple_of(group * 8 * count, 16)
        for pair in range(4):
            for q in range(TILES):
                tile = jnp.concatenate(
                    [slid[2 * pair + side, 2 * q : 2 * q + count, :] for side in range(2)], 0
                )
                sums[q] = sums[q] + summed(tile)
                win[q, pl.ds(start + pair * 2 * count, 2 * count), :] = tile.astype(BF16)
        return tuple(sums)

    window_sums = lax.fori_loop(0, chips // 8, slide, (zero,) * TILES)
    acc[0:WIDTH, :] = lax.dot_general(
        jnp.concatenate([win[q] for q in range(TILES)], 1),
        jnp.concatenate([days[r] for r in range(PHASES)], 1),
        (((0,), (0,)), ((), ())),
        preferred_element_type=F32,
    )
    acc[WIDTH:, :] = jnp.zeros((HALF, PHASES * LANES), F32)
    sums_row = jnp.concatenate([jnp.sum(s, 0, keepdims=True) for s in window_sums], 1)

    def shifted(parts):
        total = parts[0]
        lanes = lax.broadcasted_iota(jnp.int32, total.shape, 1) % HALF
        for r in range(1, PHASES):
            near = pltpu.roll(parts[r], WIDTH - KCOUNT * r, 1)
            far = pltpu.roll(parts[r], WIDTH - KCOUNT * r - (HALF - USED), 1)
            total = total + jnp.where(lanes + KCOUNT * r < USED, near, far)
        return total

    squared = jnp.sum(square_ref[...], 0, keepdims=True)
    inside = lax.broadcasted_iota(jnp.int32, (LANES, LANES), 0) % HALF
    for tile in range(TILES):
        base = tile * LANES
        total = acc[base : base + LANES, 0:LANES]
        for r in range(1, PHASES):
            lanes = slice(r * LANES, (r + 1) * LANES)
            near = base + KCOUNT * r
            far = near + HALF - USED
            total = total + jnp.where(
                inside + KCOUNT * r < USED,
                acc[near : near + LANES, lanes],
                acc[far : far + LANES, lanes],
            )
        if base <= SUM_LANE < base + LANES:
            at = lax.broadcasted_iota(jnp.int32, (LANES, LANES), 0) + base
            plain = sum(acc[base : base + LANES, r * LANES : (r + 1) * LANES] for r in range(PHASES))
            total = jnp.where(at == SUM_LANE, plain, total)
            total = jnp.where(at == SQUARE_LANE, squared, total)
        merged[:, base : base + LANES] = jnp.transpose(total)
    totals = shifted([jnp.broadcast_to(sums_row, (8, WIDTH))] * PHASES)
    kept_ref[0:HALF, :] = merged[pl.ds(pl.multiple_of(core * HALF, HALF), HALF), :]
    passed_ref[0:HALF, :] = merged[pl.ds(pl.multiple_of((1 - core) * HALF, HALF), HALF), :]
    for target in (kept_ref, passed_ref):
        target[HALF : HALF + 8, :] = totals
        target[HALF + 8 :, :] = totals


def spread(own, mine, other, square, days):
    chips, count, _ = own.shape
    return pl.pallas_call(
        spread_kernel,
        in_specs=[VMEM] * 5,
        out_specs=[VMEM] * 3,
        out_shape=[
            pltpu.VMEM((ROWS, WIDTH), F32),
            pltpu.VMEM((ROWS, WIDTH), F32),
            pltpu.VMEM((8, LANES), F32),
        ],
        scratch_shapes=[
            pltpu.VMEM((chips + 2, 16, LANES), F32),
            pltpu.VMEM((8, count + 16, LANES), F32),
            pltpu.VMEM((8, count + 16, LANES), F32),
            pltpu.VMEM((TILES, chips * count, LANES), BF16),
            pltpu.VMEM((WIDTH + HALF, PHASES * LANES), F32),
            pltpu.VMEM((LANES, WIDTH), F32),
        ],
        compiler_params=pltpu.CompilerParams(vmem_limit_bytes=32 << 20),
    )(local(own), local(mine), local(other), local(square), local(days))


def finish_kernel(
    kept_ref, taken_ref, stat_ref, lag_ref, mask_ref, offset_ref, out_ref,
    base, maps, sems, *, total_days,
):
    slots = lax.broadcasted_iota(jnp.int32, (WIDTH + 16, LANES), 0) - 16
    slot = lax.broadcasted_iota(jnp.int32, (1, LANES), 1)
    group = lax.shift_right_logical(slot * 43, 8)
    place = jnp.where(slot < TILES * 2 * PHASES, HALF * group + KCOUNT * (slot - PHASES * group), -100)
    base[...] = (slots == place).astype(F32)
    value = kept_ref[...] + taken_ref[...]
    upper = value.astype(BF16)
    rest = value - upper.astype(F32)
    middle = rest.astype(BF16)
    lower = (rest - middle.astype(F32)).astype(BF16)
    mean_x = value[0:HALF, SUM_LANE : SUM_LANE + 1] / total_days
    var_x = value[0:HALF, SQUARE_LANE : SQUARE_LANE + 1] / total_days - mean_x * mean_x
    scale_x = total_days * jnp.sqrt(var_x + 1e-06)
    scale_i = jnp.sqrt(stat_ref[1:2, :] + 1e-06)
    mask = jnp.concatenate([mask_ref[...].astype(F32), jnp.zeros((1, LANES - HALF), F32)], 1)
    mask = jnp.transpose(jnp.broadcast_to(mask, (LANES, LANES)))[0:HALF, 0:1]
    lags = lag_ref.shape[1]
    lag = jnp.concatenate([lag_ref[...], jnp.zeros((1, LANES - lags), jnp.int32)], 1)
    parts = jnp.concatenate([upper, middle, lower], 0)
    copies = []
    for pair in range(KCOUNT // 2):
        picker = jnp.concatenate(
            [base[16 - k : 16 - k + WIDTH, :].astype(BF16) for k in (2 * pair, 2 * pair + 1)], 1
        )
        thirds = jnp.dot(parts, picker, preferred_element_type=F32)
        chosen = thirds[0:ROWS] + thirds[ROWS : 2 * ROWS] + thirds[2 * ROWS :]
        for side in range(2):
            k = 2 * pair + side
            part = chosen[:, side * LANES : (side + 1) * LANES]
            wanted = BEFORE * PHASES - (lag + offset_ref[:, k : k + 1])
            part = jnp.take_along_axis(
                part, jnp.broadcast_to(wanted, part.shape), axis=1, mode="promise_in_bounds"
            )
            numer = part[0:HALF] - mean_x * part[HALF : HALF + 1]
            answer = numer / (scale_x * scale_i[:, k : k + 1]) * mask
            maps[k] = answer[:, :lags]
        copy = pltpu.make_async_copy(
            maps.at[2 * pair : 2 * pair + 2], out_ref.at[2 * pair : 2 * pair + 2], sems.at[pair]
        )
        copy.start()
        copies.append(copy)
    for copy in copies:
        copy.wait()


def finish(kept, taken, stat, lag_list, index_offset, mask, total_days):
    lags = lag_list.shape[0]
    return pl.pallas_call(
        lambda *refs: finish_kernel(*refs, total_days=total_days),
        in_specs=[VMEM] * 6,
        out_specs=ANY,
        out_shape=pltpu.HBM((KCOUNT, HALF, lags), F32),
        scratch_shapes=[
            pltpu.VMEM((WIDTH + 16, LANES), F32),
            pltpu.VMEM((KCOUNT, HALF, lags), F32),
            pltpu.SemaphoreType.DMA((KCOUNT // 2,)),
        ],
        compiler_params=SMALL,
    )(
        local(kept), local(taken), local(stat), local(lag_list[None, :]), local(mask[None, :]),
        local(index_offset[None, :]),
    )


def after(got, lag_list, index_offset, sea_mask, total_days, swapped):
    t_dev = got.shape[1] * PHASES // (PHASES + 1)
    own, mine = take_index(got, t_dev // PHASES)
    other = swapped(mine)
    days, square = middle(got, t_dev)
    kept, passed, stat = spread(own, mine, other, square, days)
    taken = swapped(passed)
    maps = finish(kept, taken, stat, lag_list, index_offset, sea_mask, total_days)
    return jnp.transpose(maps, (1, 0, 2))


def shards(field, index, lag_list, index_offset, sea_mask):
    devices = lax.axis_size(TM)
    groups = [
        [CORES * chip_at(place) + core for place in range(devices // CORES)]
        for core in range(CORES)
    ]
    got = lax.all_to_all(
        pack(field, index), TM, 0, 0, axis_index_groups=groups, tiled=True
    )
    total_days = 1.0 * index.shape[0] * devices
    swap = [(i, i ^ 1) for i in range(devices)]
    return after(
        got, lag_list, index_offset, sea_mask, total_days, lambda x: lax.ppermute(x, TM, swap)
    )


def solution(mesh):
    return jax.shard_map(
        shards,
        mesh=mesh,
        in_specs=(P(TM, None), P(TM, None), P(), P(), P(TM)),
        out_specs=P(TM, None, None),
        check_vma=False,
    )
```

```python
import jax
import jax.numpy as jnp
from jax import lax
from jax.experimental import pallas as pl
from jax.experimental.pallas import tpu as pltpu
from jax.sharding import PartitionSpec as P

TM = "tm"
CORES = 2
WEIGHTS = (1, 16, 4)
DIGITS = ((3, 2, 1, 0), (3, 2, 1, 0), (2, 3, 0, 1))
PHASES = 6
KCOUNT = 10
USED = PHASES * KCOUNT
LANES = 128
HALF = 64
BEFORE = 8
TILES = 7
WIDTH = TILES * LANES
SUM_LANE = BEFORE * HALF + USED
SQUARE_LANE = SUM_LANE + 1
ROWS = HALF + 16
STEP = 8
EARLY = 32
F32 = jnp.float32
BF16 = jnp.bfloat16
VMEM = pl.BlockSpec(memory_space=pltpu.VMEM)
ANY = pl.BlockSpec(memory_space=pl.ANY)
SMALL = pltpu.CompilerParams(vmem_limit_bytes=8 << 20)


def chip_at(place):
    chip = 0
    for i, (weight, digits) in enumerate(zip(WEIGHTS, DIGITS)):
        digit = (place >> (4 - 2 * i)) & 3
        table = sum(value << (2 * at) for at, value in enumerate(digits))
        chip = chip + weight * ((table >> (2 * digit)) & 3)
    return chip


def local(array):
    return pltpu.with_memory_space_constraint(array, pltpu.VMEM)


def fill_order(early, late):
    for target in (early, late):
        days = target.shape[0]
        length = days // PHASES
        row = lax.broadcasted_iota(jnp.int32, (length, days), 0)
        column = lax.broadcasted_iota(jnp.int32, (length, days), 1)
        for r in range(PHASES):
            target[r * length : (r + 1) * length, :] = (column == row * PHASES + r).astype(BF16)


def order_scratch(t_dev):
    ahead = EARLY * PHASES
    return [pltpu.VMEM((ahead, ahead), BF16), pltpu.VMEM((t_dev - ahead, t_dev - ahead), BF16)]


def pack_kernel(field_ref, index_ref, sent_ref, index, early, late, sems, index_sem):
    kcount, t_dev = index_ref.shape
    count = t_dev // PHASES
    chips = sent_ref.shape[0]
    ahead = EARLY * PHASES
    index_copy = pltpu.make_async_copy(index_ref, index, index_sem)
    index_copy.start()

    def copy(place):
        lanes = pl.ds(pl.multiple_of(chip_at(place) * LANES, LANES), LANES)
        return pltpu.make_async_copy(
            field_ref.at[:, lanes], sent_ref.at[place, 0:t_dev, :], sems.at[place]
        )

    def start(place, _):
        copy(place).start()
        return 0

    lax.fori_loop(0, chips, start, 0, unroll=8)
    fill_order(early, late)
    index_copy.wait()
    rest = index[...]
    value = jnp.zeros((count, USED), F32)
    for _ in range(3):
        part = rest.astype(BF16)
        rest = rest - part.astype(F32)
        first = lax.dot_general(
            early[...], part[:, :ahead], (((1,), (1,)), ((), ())), preferred_element_type=F32
        )
        second = lax.dot_general(
            late[...], part[:, ahead:], (((1,), (1,)), ((), ())), preferred_element_type=F32
        )
        later = count - EARLY
        value = value + jnp.concatenate(
            [
                jnp.concatenate(
                    [first[r * EARLY : (r + 1) * EARLY], second[r * later : (r + 1) * later]], 0
                )
                for r in range(PHASES)
            ],
            1,
        )
    origin = value[0:1].astype(BF16).astype(F32)
    top = lax.broadcasted_iota(jnp.int32, value.shape, 0) == 0
    value = jnp.where(top, value, value - origin)
    upper = value.astype(BF16).astype(F32)
    blank = jnp.zeros((count, HALF - USED), F32)
    rows = jnp.concatenate([upper, blank, value - upper, blank], 1).astype(BF16)

    def repeat(place, _):
        sent_ref[place, t_dev:, :] = rows
        return 0

    lax.fori_loop(0, chips, repeat, 0, unroll=8)

    def finish_copy(place, _):
        copy(place).wait()
        return 0

    lax.fori_loop(0, chips, finish_copy, 0, unroll=8)


def pack(field, index):
    t_dev, cells = field.shape
    chips = cells // LANES
    return pl.pallas_call(
        pack_kernel,
        in_specs=[ANY] * 2,
        out_specs=VMEM,
        out_shape=pltpu.VMEM((chips, t_dev + t_dev // PHASES, LANES), BF16),
        scratch_shapes=[pltpu.VMEM(index.T.shape, F32)]
        + order_scratch(t_dev)
        + [pltpu.SemaphoreType.DMA((chips,)), pltpu.SemaphoreType.DMA],
        compiler_params=SMALL,
    )(*[pltpu.with_memory_space_constraint(x, pltpu.HBM) for x in (field, index.T)])


def joined(raw):
    wide = raw.astype(F32)
    turned = pltpu.roll(wide, HALF, 1)
    value = wide + turned
    lane = lax.broadcasted_iota(jnp.int32, (1, LANES), 1)
    origin = jnp.where(lane < HALF, wide[0:1], turned[0:1])
    top = lax.broadcasted_iota(jnp.int32, value.shape, 0) == 0
    return jnp.where(top, value, value + origin)


def summed(value):
    return jnp.sum(value.reshape(-1, 8, LANES), 0)


def take_kernel(got_ref, own_ref, edge_ref):
    chips, count, _ = own_ref.shape
    zero = jnp.zeros((8, LANES), F32)

    def body(place, sums):
        first, second = sums
        chip = chip_at(place)
        value = joined(got_ref[place, PHASES * count :, :])
        own_ref[place] = value
        edge_ref[chip, 0:8, :] = value[0:8]
        edge_ref[chip, 8:16, :] = value[count - 8 :]
        return first + summed(value), second + summed(value * value)

    first, second = lax.fori_loop(0, chips, body, (zero, zero), unroll=16)
    edge_ref[chips, 0:8, :] = first
    edge_ref[chips, 8:16, :] = second


def take_index(got, count):
    chips = got.shape[0]
    return pl.pallas_call(
        take_kernel,
        in_specs=[VMEM],
        out_specs=[VMEM] * 2,
        out_shape=[
            pltpu.VMEM((chips, count, LANES), F32),
            pltpu.VMEM((chips + 1, 16, LANES), F32),
        ],
        compiler_params=SMALL,
    )(local(got))


def middle_kernel(got_ref, days_ref, square_ref, early, late):
    chips, rows, _ = got_ref.shape
    t_dev = rows * PHASES // (PHASES + 1)
    count = t_dev // PHASES
    ahead = EARLY * PHASES
    fill_order(early, late)

    def body(pair, square):
        start = pl.multiple_of(pair * 2 * count, 16)
        for source, days, base in ((early, slice(0, ahead), 0), (late, slice(ahead, t_dev), EARLY)):
            length = source.shape[0] // PHASES
            blocks = [got_ref[2 * pair + side, days, :] for side in range(2)]
            for block in blocks:
                wide = block.astype(F32)
                square = square + jnp.sum((wide * wide).reshape(-1, 16, LANES), 0)
            mixed = jnp.dot(
                source[...], jnp.concatenate(blocks, 1), preferred_element_type=F32
            )
            for r in range(PHASES):
                piece = mixed[r * length : (r + 1) * length].astype(BF16)
                days_ref[r, pl.ds(start + base, length), :] = piece[:, :LANES]
                days_ref[r, pl.ds(start + count + base, length), :] = piece[:, LANES:]
        return square

    square_ref[...] = lax.fori_loop(0, chips // 2, body, jnp.zeros((16, LANES), F32), unroll=8)


def middle(got, t_dev):
    chips = got.shape[0]
    return pl.pallas_call(
        middle_kernel,
        in_specs=[VMEM],
        out_specs=[VMEM] * 2,
        out_shape=[
            pltpu.VMEM((PHASES, chips * t_dev // PHASES, LANES), BF16),
            pltpu.VMEM((16, LANES), F32),
        ],
        scratch_shapes=order_scratch(t_dev),
        compiler_params=SMALL,
    )(local(got))


def spread_kernel(
    own, mine_ref, other_ref, square_ref, days,
    kept_ref, passed_ref, stat_ref,
    edge, line, slid, win, late_win, acc, merged,
):
    chips, count, _ = own.shape
    core = lax.rem(lax.axis_index(TM), CORES)
    total_days = 2.0 * chips * count * PHASES
    zero = jnp.zeros((8, LANES), F32)
    sums = mine_ref[chips] + other_ref[chips]
    row = lax.broadcasted_iota(jnp.int32, (LANES, LANES), 0)
    column = lax.broadcasted_iota(jnp.int32, (LANES, LANES), 1) % HALF
    same = (row < USED) & (column < USED) & (row % KCOUNT == column % KCOUNT)
    folded = jnp.dot(
        sums, same.astype(F32), precision=lax.Precision.HIGHEST, preferred_element_type=F32
    )
    mean = jnp.sum(folded[0:8], 0, keepdims=True) / total_days
    var = jnp.sum(folded[8:16], 0, keepdims=True) / total_days - mean * mean
    stat_ref[...] = jnp.concatenate([mean, var, jnp.zeros((6, LANES), F32)], 0)
    lane = lax.broadcasted_iota(jnp.int32, (1, LANES), 1)
    valid = lane % HALF < USED

    def centered(value):
        return jnp.where(valid, (value - mean).astype(BF16).astype(F32), 0.0)

    edge[0] = jnp.broadcast_to(mean, (16, LANES))
    edge[chips + 1] = jnp.broadcast_to(mean, (16, LANES))

    def move(chip, _):
        edge[chip + 1] = other_ref[chip]
        return 0

    lax.fori_loop(0, chips, move, 0, unroll=16)

    def slide(group, sums, target, offset, base):
        sums = list(sums)
        for side in range(8):
            place = 8 * group + side
            chip = chip_at(place)
            at = base + side
            line[at, 0:8, :] = centered(edge[chip + core, 8:16, :])
            line[at, 8 : 8 + count, :] = jnp.where(lane == USED, 1.0, centered(own[place]))
            line[at, 8 + count :, :] = centered(edge[chip + core + 1, 0:8, :])
            sums[0] = sums[0] + line[at, 0:16, :] - line[at, count : count + 16, :]
            sums[1] = sums[1] + summed(line[at, 8 : 8 + count, :])
        for side in range(8):
            at = base + side
            slid[at, 0 : count + 15, :] = jnp.where(
                lane < HALF, line[at, 0 : count + 15, :], line[at, 1 : count + 16, :]
            )
        start = (8 * group - offset) * count
        if not isinstance(start, int):
            start = pl.multiple_of(start, 16)
        for pair in range(8 // 2):
            for q in range(TILES):
                tile = jnp.concatenate(
                    [slid[base + 2 * pair + side, 2 * q : 2 * q + count, :] for side in range(2)], 0
                )
                target[q, pl.ds(start + pair * 2 * count, 2 * count), :] = tile.astype(BF16)
        return tuple(sums)

    def multiply(source, rows):
        return lax.dot_general(
            jnp.concatenate([source[q] for q in range(TILES)], 1),
            jnp.concatenate([days[r, rows, :] for r in range(PHASES)], 1),
            (((0,), (0,)), ((), ())),
            preferred_element_type=F32,
        )

    half = chips // 2
    window_sums = lax.fori_loop(
        0, half // 8, lambda g, sums: slide(g, sums, win, 0, 0), (jnp.zeros((16, LANES), F32), zero)
    )
    acc[0:WIDTH, :] = multiply(win, slice(0, half * count))
    for group in range(half // 8, chips // 8):
        window_sums = slide(group, window_sums, late_win, half, 8 * (group % 2))
    acc[0:WIDTH, :] += multiply(late_win, slice(half * count, chips * count))
    edges, inner = window_sums
    acc[WIDTH:, :] = jnp.zeros((HALF, PHASES * LANES), F32)
    inner = jnp.sum(inner, 0, keepdims=True)
    at = lax.broadcasted_iota(jnp.int32, (16, LANES), 0)
    upper_half = (lax.broadcasted_iota(jnp.int32, (16, LANES), 1) >= HALF).astype(jnp.int32)
    window_sums = []
    for q in range(TILES):
        move = 2 * q - BEFORE + upper_half
        gained = (at >= 8 + move) & (at < 8)
        lost = (at >= 8) & (at < 8 + move)
        change = jnp.where(gained, edges, 0.0) - jnp.where(lost, edges, 0.0)
        window_sums.append(inner + jnp.sum(change, 0, keepdims=True))
    sums_row = jnp.concatenate(window_sums, 1)

    def shifted(parts):
        total = parts[0]
        lanes = lax.broadcasted_iota(jnp.int32, total.shape, 1) % HALF
        for r in range(1, PHASES):
            near = pltpu.roll(parts[r], WIDTH - KCOUNT * r, 1)
            far = pltpu.roll(parts[r], WIDTH - KCOUNT * r - (HALF - USED), 1)
            total = total + jnp.where(lanes + KCOUNT * r < USED, near, far)
        return total

    squared = jnp.sum(square_ref[...], 0, keepdims=True)
    inside = lax.broadcasted_iota(jnp.int32, (LANES, LANES), 0) % HALF
    for tile in range(TILES):
        base = tile * LANES
        total = acc[base : base + LANES, 0:LANES]
        for r in range(1, PHASES):
            lanes = slice(r * LANES, (r + 1) * LANES)
            near = base + KCOUNT * r
            far = near + HALF - USED
            total = total + jnp.where(
                inside + KCOUNT * r < USED,
                acc[near : near + LANES, lanes],
                acc[far : far + LANES, lanes],
            )
        if base <= SUM_LANE < base + LANES:
            at = lax.broadcasted_iota(jnp.int32, (LANES, LANES), 0) + base
            plain = sum(acc[base : base + LANES, r * LANES : (r + 1) * LANES] for r in range(PHASES))
            total = jnp.where(at == SUM_LANE, plain, total)
            total = jnp.where(at == SQUARE_LANE, squared, total)
        merged[:, base : base + LANES] = jnp.transpose(total)
    totals = shifted([jnp.broadcast_to(sums_row, (8, WIDTH))] * PHASES)
    kept_ref[0:HALF, :] = merged[pl.ds(pl.multiple_of(core * HALF, HALF), HALF), :]
    passed_ref[0:HALF, :] = merged[pl.ds(pl.multiple_of((1 - core) * HALF, HALF), HALF), :]
    for target in (kept_ref, passed_ref):
        target[HALF : HALF + 8, :] = totals
        target[HALF + 8 :, :] = totals


def spread(own, mine, other, square, days):
    chips, count, _ = own.shape
    return pl.pallas_call(
        spread_kernel,
        in_specs=[VMEM] * 5,
        out_specs=[VMEM] * 3,
        out_shape=[
            pltpu.VMEM((ROWS, WIDTH), F32),
            pltpu.VMEM((ROWS, WIDTH), F32),
            pltpu.VMEM((8, LANES), F32),
        ],
        scratch_shapes=[
            pltpu.VMEM((chips + 2, 16, LANES), F32),
            pltpu.VMEM((16, count + 16, LANES), F32),
            pltpu.VMEM((16, count + 16, LANES), F32),
            pltpu.VMEM((TILES, chips * count // 2, LANES), BF16),
            pltpu.VMEM((TILES, chips * count // 2, LANES), BF16),
            pltpu.VMEM((WIDTH + HALF, PHASES * LANES), F32),
            pltpu.VMEM((LANES, WIDTH), F32),
        ],
        compiler_params=pltpu.CompilerParams(vmem_limit_bytes=32 << 20),
    )(local(own), local(mine), local(other), local(square), local(days))


def finish_kernel(
    kept_ref, taken_ref, stat_ref, lag_ref, mask_ref, offset_ref, out_ref,
    base, maps, sems, *, total_days,
):
    slots = lax.broadcasted_iota(jnp.int32, (WIDTH + 16, LANES), 0) - 16
    slot = lax.broadcasted_iota(jnp.int32, (1, LANES), 1)
    group = lax.shift_right_logical(slot * 43, 8)
    place = jnp.where(slot < TILES * 2 * PHASES, HALF * group + KCOUNT * (slot - PHASES * group), -100)
    base[...] = (slots == place).astype(F32)
    value = kept_ref[...] + taken_ref[...]
    upper = value.astype(BF16)
    rest = value - upper.astype(F32)
    middle = rest.astype(BF16)
    lower = (rest - middle.astype(F32)).astype(BF16)
    mean_x = value[0:HALF, SUM_LANE : SUM_LANE + 1] / total_days
    var_x = value[0:HALF, SQUARE_LANE : SQUARE_LANE + 1] / total_days - mean_x * mean_x
    scale_x = total_days * jnp.sqrt(var_x + 1e-06)
    scale_i = jnp.sqrt(stat_ref[1:2, :] + 1e-06)
    mask = jnp.concatenate([mask_ref[...].astype(F32), jnp.zeros((1, LANES - HALF), F32)], 1)
    mask = jnp.transpose(jnp.broadcast_to(mask, (LANES, LANES)))[0:HALF, 0:1]
    lags = lag_ref.shape[1]
    lag = jnp.concatenate([lag_ref[...], jnp.zeros((1, LANES - lags), jnp.int32)], 1)
    parts = jnp.concatenate([upper, middle, lower], 0)
    copies = []
    for pair in range(KCOUNT // 2):
        picker = jnp.concatenate(
            [base[16 - k : 16 - k + WIDTH, :].astype(BF16) for k in (2 * pair, 2 * pair + 1)], 1
        )
        thirds = jnp.dot(parts, picker, preferred_element_type=F32)
        chosen = thirds[0:ROWS] + thirds[ROWS : 2 * ROWS] + thirds[2 * ROWS :]
        for side in range(2):
            k = 2 * pair + side
            part = chosen[:, side * LANES : (side + 1) * LANES]
            wanted = BEFORE * PHASES - (lag + offset_ref[:, k : k + 1])
            part = jnp.take_along_axis(
                part, jnp.broadcast_to(wanted, part.shape), axis=1, mode="promise_in_bounds"
            )
            numer = part[0:HALF] - mean_x * part[HALF : HALF + 1]
            answer = numer / (scale_x * scale_i[:, k : k + 1]) * mask
            maps[k] = answer[:, :lags]
        copy = pltpu.make_async_copy(
            maps.at[2 * pair : 2 * pair + 2], out_ref.at[2 * pair : 2 * pair + 2], sems.at[pair]
        )
        copy.start()
        copies.append(copy)
    for copy in copies:
        copy.wait()


def finish(kept, taken, stat, lag_list, index_offset, mask, total_days):
    lags = lag_list.shape[0]
    return pl.pallas_call(
        lambda *refs: finish_kernel(*refs, total_days=total_days),
        in_specs=[VMEM] * 6,
        out_specs=ANY,
        out_shape=pltpu.HBM((KCOUNT, HALF, lags), F32),
        scratch_shapes=[
            pltpu.VMEM((WIDTH + 16, LANES), F32),
            pltpu.VMEM((KCOUNT, HALF, lags), F32),
            pltpu.SemaphoreType.DMA((KCOUNT // 2,)),
        ],
        compiler_params=SMALL,
    )(
        local(kept), local(taken), local(stat), local(lag_list[None, :]), local(mask[None, :]),
        local(index_offset[None, :]),
    )


def after(got, lag_list, index_offset, sea_mask, total_days, swapped):
    t_dev = got.shape[1] * PHASES // (PHASES + 1)
    own, mine = take_index(got, t_dev // PHASES)
    other = swapped(mine)
    days, square = middle(got, t_dev)
    kept, passed, stat = spread(own, mine, other, square, days)
    taken = swapped(passed)
    maps = finish(kept, taken, stat, lag_list, index_offset, sea_mask, total_days)
    return jnp.transpose(maps, (1, 0, 2))


def shards(field, index, lag_list, index_offset, sea_mask):
    devices = lax.axis_size(TM)
    groups = [
        [CORES * chip_at(place) + core for place in range(devices // CORES)]
        for core in range(CORES)
    ]
    got = lax.all_to_all(
        pack(field, index), TM, 0, 0, axis_index_groups=groups, tiled=True
    )
    total_days = 1.0 * index.shape[0] * devices
    swap = [(i, i ^ 1) for i in range(devices)]
    return after(
        got, lag_list, index_offset, sea_mask, total_days, lambda x: lax.ppermute(x, TM, swap)
    )


def solution(mesh):
    return jax.shard_map(
        shards,
        mesh=mesh,
        in_specs=(P(TM, None), P(TM, None), P(), P(), P(TM)),
        out_specs=P(TM, None, None),
        check_vma=False,
    )
```

```python
import jax
import jax.numpy as jnp
from jax import lax
from jax.experimental import pallas as pl
from jax.experimental.pallas import tpu as pltpu
from jax.sharding import PartitionSpec as P

TM = "tm"
CORES = 2
WEIGHTS = (1, 16, 4)
DIGITS = ((3, 2, 1, 0), (3, 2, 1, 0), (2, 3, 0, 1))
PHASES = 6
KCOUNT = 10
USED = PHASES * KCOUNT
LANES = 128
HALF = 64
BEFORE = 8
TILES = 7
WIDTH = TILES * LANES
SUM_LANE = BEFORE * HALF + USED
SQUARE_LANE = SUM_LANE + 1
ROWS = HALF + 16
STEP = 8
EARLY = 32
F32 = jnp.float32
BF16 = jnp.bfloat16
VMEM = pl.BlockSpec(memory_space=pltpu.VMEM)
ANY = pl.BlockSpec(memory_space=pl.ANY)
SMALL = pltpu.CompilerParams(vmem_limit_bytes=8 << 20)


def chip_at(place):
    chip = 0
    for i, (weight, digits) in enumerate(zip(WEIGHTS, DIGITS)):
        digit = (place >> (4 - 2 * i)) & 3
        table = sum(value << (2 * at) for at, value in enumerate(digits))
        chip = chip + weight * ((table >> (2 * digit)) & 3)
    return chip


def local(array):
    return pltpu.with_memory_space_constraint(array, pltpu.VMEM)


def fill_order(early, late):
    for target in (early, late):
        days = target.shape[0]
        length = days // PHASES
        row = lax.broadcasted_iota(jnp.int32, (length, days), 0)
        column = lax.broadcasted_iota(jnp.int32, (length, days), 1)
        for r in range(PHASES):
            target[r * length : (r + 1) * length, :] = (column == row * PHASES + r).astype(BF16)


def order_scratch(t_dev):
    ahead = EARLY * PHASES
    return [pltpu.VMEM((ahead, ahead), BF16), pltpu.VMEM((t_dev - ahead, t_dev - ahead), BF16)]


def pack_kernel(field_ref, index_ref, sent_ref, index, early, late, sems, index_sem):
    kcount, t_dev = index_ref.shape
    count = t_dev // PHASES
    chips = sent_ref.shape[0]
    ahead = EARLY * PHASES
    index_copy = pltpu.make_async_copy(index_ref, index, index_sem)
    index_copy.start()

    def copy(place):
        lanes = pl.ds(pl.multiple_of(chip_at(place) * LANES, LANES), LANES)
        return pltpu.make_async_copy(
            field_ref.at[:, lanes], sent_ref.at[place, 0:t_dev, :], sems.at[place]
        )

    def start(place, _):
        copy(place).start()
        return 0

    lax.fori_loop(0, chips, start, 0, unroll=8)
    fill_order(early, late)
    index_copy.wait()
    rest = index[...]
    value = jnp.zeros((count, USED), F32)
    for _ in range(3):
        part = rest.astype(BF16)
        rest = rest - part.astype(F32)
        first = lax.dot_general(
            early[...], part[:, :ahead], (((1,), (1,)), ((), ())), preferred_element_type=F32
        )
        second = lax.dot_general(
            late[...], part[:, ahead:], (((1,), (1,)), ((), ())), preferred_element_type=F32
        )
        later = count - EARLY
        value = value + jnp.concatenate(
            [
                jnp.concatenate(
                    [first[r * EARLY : (r + 1) * EARLY], second[r * later : (r + 1) * later]], 0
                )
                for r in range(PHASES)
            ],
            1,
        )
    origin = value[0:1].astype(BF16).astype(F32)
    top = lax.broadcasted_iota(jnp.int32, value.shape, 0) == 0
    value = jnp.where(top, value, value - origin)
    upper = value.astype(BF16).astype(F32)
    blank = jnp.zeros((count, HALF - USED), F32)
    rows = jnp.concatenate([upper, blank, value - upper, blank], 1).astype(BF16)

    def repeat(place, _):
        sent_ref[place, t_dev:, :] = rows
        return 0

    lax.fori_loop(0, chips, repeat, 0, unroll=8)

    def finish_copy(place, _):
        copy(place).wait()
        return 0

    lax.fori_loop(0, chips, finish_copy, 0, unroll=8)


def pack(field, index):
    t_dev, cells = field.shape
    chips = cells // LANES
    return pl.pallas_call(
        pack_kernel,
        in_specs=[ANY] * 2,
        out_specs=VMEM,
        out_shape=pltpu.VMEM((chips, t_dev + t_dev // PHASES, LANES), BF16),
        scratch_shapes=[pltpu.VMEM(index.T.shape, F32)]
        + order_scratch(t_dev)
        + [pltpu.SemaphoreType.DMA((chips,)), pltpu.SemaphoreType.DMA],
        compiler_params=SMALL,
    )(*[pltpu.with_memory_space_constraint(x, pltpu.HBM) for x in (field, index.T)])


def joined(raw):
    wide = raw.astype(F32)
    turned = pltpu.roll(wide, HALF, 1)
    value = wide + turned
    lane = lax.broadcasted_iota(jnp.int32, (1, LANES), 1)
    origin = jnp.where(lane < HALF, wide[0:1], turned[0:1])
    top = lax.broadcasted_iota(jnp.int32, value.shape, 0) == 0
    return jnp.where(top, value, value + origin)


def summed(value):
    return jnp.sum(value.reshape(-1, 8, LANES), 0)


def take_kernel(got_ref, own_ref, edge_ref):
    chips, count, _ = own_ref.shape
    zero = jnp.zeros((8, LANES), F32)

    def body(place, sums):
        first, second = sums
        chip = chip_at(place)
        value = joined(got_ref[place, PHASES * count :, :])
        own_ref[place] = value
        edge_ref[chip, 0:8, :] = value[0:8]
        edge_ref[chip, 8:16, :] = value[count - 8 :]
        return first + summed(value), second + summed(value * value)

    first, second = lax.fori_loop(0, chips, body, (zero, zero), unroll=32)
    edge_ref[chips, 0:8, :] = first
    edge_ref[chips, 8:16, :] = second


def take_index(got, count):
    chips = got.shape[0]
    return pl.pallas_call(
        take_kernel,
        in_specs=[VMEM],
        out_specs=[VMEM] * 2,
        out_shape=[
            pltpu.VMEM((chips, count, LANES), F32),
            pltpu.VMEM((chips + 1, 16, LANES), F32),
        ],
        compiler_params=SMALL,
    )(local(got))


def middle_kernel(got_ref, days_ref, square_ref, early, late):
    chips, rows, _ = got_ref.shape
    t_dev = rows * PHASES // (PHASES + 1)
    count = t_dev // PHASES
    ahead = EARLY * PHASES
    fill_order(early, late)

    def body(pair, square):
        start = pl.multiple_of(pair * 2 * count, 16)
        for source, days, base in ((early, slice(0, ahead), 0), (late, slice(ahead, t_dev), EARLY)):
            length = source.shape[0] // PHASES
            blocks = [got_ref[2 * pair + side, days, :] for side in range(2)]
            for block in blocks:
                wide = block.astype(F32)
                square = square + jnp.sum((wide * wide).reshape(-1, 16, LANES), 0)
            mixed = jnp.dot(
                source[...], jnp.concatenate(blocks, 1), preferred_element_type=F32
            )
            for r in range(PHASES):
                piece = mixed[r * length : (r + 1) * length].astype(BF16)
                days_ref[r, pl.ds(start + base, length), :] = piece[:, :LANES]
                days_ref[r, pl.ds(start + count + base, length), :] = piece[:, LANES:]
        return square

    square_ref[...] = lax.fori_loop(0, chips // 2, body, jnp.zeros((16, LANES), F32), unroll=16)


def middle(got, t_dev):
    chips = got.shape[0]
    return pl.pallas_call(
        middle_kernel,
        in_specs=[VMEM],
        out_specs=[VMEM] * 2,
        out_shape=[
            pltpu.VMEM((PHASES, chips * t_dev // PHASES, LANES), BF16),
            pltpu.VMEM((16, LANES), F32),
        ],
        scratch_shapes=order_scratch(t_dev),
        compiler_params=SMALL,
    )(local(got))


def spread_kernel(
    own, mine_ref, other_ref, square_ref, days,
    kept_ref, passed_ref, stat_ref,
    edge, line, slid, win, late_win, acc, merged,
):
    chips, count, _ = own.shape
    core = lax.rem(lax.axis_index(TM), CORES)
    total_days = 2.0 * chips * count * PHASES
    zero = jnp.zeros((8, LANES), F32)
    sums = mine_ref[chips] + other_ref[chips]
    row = lax.broadcasted_iota(jnp.int32, (LANES, LANES), 0)
    column = lax.broadcasted_iota(jnp.int32, (LANES, LANES), 1) % HALF
    same = (row < USED) & (column < USED) & (row % KCOUNT == column % KCOUNT)
    folded = jnp.dot(
        sums, same.astype(F32), precision=lax.Precision.HIGHEST, preferred_element_type=F32
    )
    mean = jnp.sum(folded[0:8], 0, keepdims=True) / total_days
    var = jnp.sum(folded[8:16], 0, keepdims=True) / total_days - mean * mean
    stat_ref[...] = jnp.concatenate([mean, var, jnp.zeros((6, LANES), F32)], 0)
    lane = lax.broadcasted_iota(jnp.int32, (1, LANES), 1)
    valid = lane % HALF < USED

    def centered(value):
        return jnp.where(valid, (value - mean).astype(BF16).astype(F32), 0.0)

    edge[0] = jnp.broadcast_to(mean, (16, LANES))
    edge[chips + 1] = jnp.broadcast_to(mean, (16, LANES))

    def move(chip, _):
        edge[chip + 1] = other_ref[chip]
        return 0

    lax.fori_loop(0, chips, move, 0, unroll=16)

    def slide(group, sums, target, offset, base):
        sums = list(sums)
        for side in range(8):
            place = 8 * group + side
            chip = chip_at(place)
            at = base + side
            line[at, 0:8, :] = centered(edge[chip + core, 8:16, :])
            line[at, 8 : 8 + count, :] = jnp.where(lane == USED, 1.0, centered(own[place]))
            line[at, 8 + count :, :] = centered(edge[chip + core + 1, 0:8, :])
            sums[0] = sums[0] + line[at, 0:16, :] - line[at, count : count + 16, :]
            sums[1] = sums[1] + summed(line[at, 8 : 8 + count, :])
        for side in range(8):
            at = base + side
            slid[at, 0 : count + 15, :] = jnp.where(
                lane < HALF, line[at, 0 : count + 15, :], line[at, 1 : count + 16, :]
            )
        start = (8 * group - offset) * count
        if not isinstance(start, int):
            start = pl.multiple_of(start, 16)
        for pair in range(8 // 2):
            for q in range(TILES):
                tile = jnp.concatenate(
                    [slid[base + 2 * pair + side, 2 * q : 2 * q + count, :] for side in range(2)], 0
                )
                target[q, pl.ds(start + pair * 2 * count, 2 * count), :] = tile.astype(BF16)
        return tuple(sums)

    def multiply(source, rows):
        return lax.dot_general(
            jnp.concatenate([source[q] for q in range(TILES)], 1),
            jnp.concatenate([days[r, rows, :] for r in range(PHASES)], 1),
            (((0,), (0,)), ((), ())),
            preferred_element_type=F32,
        )

    half = chips // 2
    window_sums = lax.fori_loop(
        0, half // 8, lambda g, sums: slide(g, sums, win, 0, 0), (jnp.zeros((16, LANES), F32), zero)
    )
    acc[0:WIDTH, :] = multiply(win, slice(0, half * count))
    for group in range(half // 8, chips // 8):
        window_sums = slide(group, window_sums, late_win, half, 8 * (group % 2))
    acc[0:WIDTH, :] += multiply(late_win, slice(half * count, chips * count))
    edges, inner = window_sums
    acc[WIDTH:, :] = jnp.zeros((HALF, PHASES * LANES), F32)
    inner = jnp.sum(inner, 0, keepdims=True)
    at = lax.broadcasted_iota(jnp.int32, (16, LANES), 0)
    upper_half = (lax.broadcasted_iota(jnp.int32, (16, LANES), 1) >= HALF).astype(jnp.int32)
    window_sums = []
    for q in range(TILES):
        move = 2 * q - BEFORE + upper_half
        gained = (at >= 8 + move) & (at < 8)
        lost = (at >= 8) & (at < 8 + move)
        change = jnp.where(gained, edges, 0.0) - jnp.where(lost, edges, 0.0)
        window_sums.append(inner + jnp.sum(change, 0, keepdims=True))
    sums_row = jnp.concatenate(window_sums, 1)

    def shifted(parts):
        total = parts[0]
        lanes = lax.broadcasted_iota(jnp.int32, total.shape, 1) % HALF
        for r in range(1, PHASES):
            near = pltpu.roll(parts[r], WIDTH - KCOUNT * r, 1)
            far = pltpu.roll(parts[r], WIDTH - KCOUNT * r - (HALF - USED), 1)
            total = total + jnp.where(lanes + KCOUNT * r < USED, near, far)
        return total

    squared = jnp.sum(square_ref[...], 0, keepdims=True)
    inside = lax.broadcasted_iota(jnp.int32, (LANES, LANES), 0) % HALF
    for tile in range(TILES):
        base = tile * LANES
        total = acc[base : base + LANES, 0:LANES]
        for r in range(1, PHASES):
            lanes = slice(r * LANES, (r + 1) * LANES)
            near = base + KCOUNT * r
            far = near + HALF - USED
            total = total + jnp.where(
                inside + KCOUNT * r < USED,
                acc[near : near + LANES, lanes],
                acc[far : far + LANES, lanes],
            )
        if base <= SUM_LANE < base + LANES:
            at = lax.broadcasted_iota(jnp.int32, (LANES, LANES), 0) + base
            plain = sum(acc[base : base + LANES, r * LANES : (r + 1) * LANES] for r in range(PHASES))
            total = jnp.where(at == SUM_LANE, plain, total)
            total = jnp.where(at == SQUARE_LANE, squared, total)
        merged[:, base : base + LANES] = jnp.transpose(total)
    totals = shifted([jnp.broadcast_to(sums_row, (8, WIDTH))] * PHASES)
    kept_ref[0:HALF, :] = merged[pl.ds(pl.multiple_of(core * HALF, HALF), HALF), :]
    passed_ref[0:HALF, :] = merged[pl.ds(pl.multiple_of((1 - core) * HALF, HALF), HALF), :]
    for target in (kept_ref, passed_ref):
        target[HALF : HALF + 8, :] = totals
        target[HALF + 8 :, :] = totals


def spread(own, mine, other, square, days):
    chips, count, _ = own.shape
    return pl.pallas_call(
        spread_kernel,
        in_specs=[VMEM] * 5,
        out_specs=[VMEM] * 3,
        out_shape=[
            pltpu.VMEM((ROWS, WIDTH), F32),
            pltpu.VMEM((ROWS, WIDTH), F32),
            pltpu.VMEM((8, LANES), F32),
        ],
        scratch_shapes=[
            pltpu.VMEM((chips + 2, 16, LANES), F32),
            pltpu.VMEM((16, count + 16, LANES), F32),
            pltpu.VMEM((16, count + 16, LANES), F32),
            pltpu.VMEM((TILES, chips * count // 2, LANES), BF16),
            pltpu.VMEM((TILES, chips * count // 2, LANES), BF16),
            pltpu.VMEM((WIDTH + HALF, PHASES * LANES), F32),
            pltpu.VMEM((LANES, WIDTH), F32),
        ],
        compiler_params=pltpu.CompilerParams(vmem_limit_bytes=32 << 20),
    )(local(own), local(mine), local(other), local(square), local(days))


def finish_kernel(
    kept_ref, taken_ref, stat_ref, lag_ref, mask_ref, offset_ref, out_ref,
    base, maps, sems, *, total_days,
):
    slots = lax.broadcasted_iota(jnp.int32, (WIDTH + 16, LANES), 0) - 16
    slot = lax.broadcasted_iota(jnp.int32, (1, LANES), 1)
    group = lax.shift_right_logical(slot * 43, 8)
    place = jnp.where(slot < TILES * 2 * PHASES, HALF * group + KCOUNT * (slot - PHASES * group), -100)
    base[...] = (slots == place).astype(F32)
    value = kept_ref[...] + taken_ref[...]
    upper = value.astype(BF16)
    rest = value - upper.astype(F32)
    middle = rest.astype(BF16)
    lower = (rest - middle.astype(F32)).astype(BF16)
    mean_x = value[0:HALF, SUM_LANE : SUM_LANE + 1] / total_days
    var_x = value[0:HALF, SQUARE_LANE : SQUARE_LANE + 1] / total_days - mean_x * mean_x
    scale_x = total_days * jnp.sqrt(var_x + 1e-06)
    scale_i = jnp.sqrt(stat_ref[1:2, :] + 1e-06)
    mask = jnp.concatenate([mask_ref[...].astype(F32), jnp.zeros((1, LANES - HALF), F32)], 1)
    mask = jnp.transpose(jnp.broadcast_to(mask, (LANES, LANES)))[0:HALF, 0:1]
    lags = lag_ref.shape[1]
    lag = jnp.concatenate([lag_ref[...], jnp.zeros((1, LANES - lags), jnp.int32)], 1)
    parts = jnp.concatenate([upper, middle, lower], 0)
    copies = []
    for pair in range(KCOUNT // 2):
        picker = jnp.concatenate(
            [base[16 - k : 16 - k + WIDTH, :].astype(BF16) for k in (2 * pair, 2 * pair + 1)], 1
        )
        thirds = jnp.dot(parts, picker, preferred_element_type=F32)
        chosen = thirds[0:ROWS] + thirds[ROWS : 2 * ROWS] + thirds[2 * ROWS :]
        for side in range(2):
            k = 2 * pair + side
            part = chosen[:, side * LANES : (side + 1) * LANES]
            wanted = BEFORE * PHASES - (lag + offset_ref[:, k : k + 1])
            part = jnp.take_along_axis(
                part, jnp.broadcast_to(wanted, part.shape), axis=1, mode="promise_in_bounds"
            )
            numer = part[0:HALF] - mean_x * part[HALF : HALF + 1]
            answer = numer / (scale_x * scale_i[:, k : k + 1]) * mask
            maps[k] = answer[:, :lags]
        copy = pltpu.make_async_copy(
            maps.at[2 * pair : 2 * pair + 2], out_ref.at[2 * pair : 2 * pair + 2], sems.at[pair]
        )
        copy.start()
        copies.append(copy)
    for copy in copies:
        copy.wait()


def finish(kept, taken, stat, lag_list, index_offset, mask, total_days):
    lags = lag_list.shape[0]
    return pl.pallas_call(
        lambda *refs: finish_kernel(*refs, total_days=total_days),
        in_specs=[VMEM] * 6,
        out_specs=ANY,
        out_shape=pltpu.HBM((KCOUNT, HALF, lags), F32),
        scratch_shapes=[
            pltpu.VMEM((WIDTH + 16, LANES), F32),
            pltpu.VMEM((KCOUNT, HALF, lags), F32),
            pltpu.SemaphoreType.DMA((KCOUNT // 2,)),
        ],
        compiler_params=SMALL,
    )(
        local(kept), local(taken), local(stat), local(lag_list[None, :]), local(mask[None, :]),
        local(index_offset[None, :]),
    )


def after(got, lag_list, index_offset, sea_mask, total_days, swapped):
    t_dev = got.shape[1] * PHASES // (PHASES + 1)
    own, mine = take_index(got, t_dev // PHASES)
    other = swapped(mine)
    days, square = middle(got, t_dev)
    kept, passed, stat = spread(own, mine, other, square, days)
    taken = swapped(passed)
    maps = finish(kept, taken, stat, lag_list, index_offset, sea_mask, total_days)
    return jnp.transpose(maps, (1, 0, 2))


def shards(field, index, lag_list, index_offset, sea_mask):
    devices = lax.axis_size(TM)
    groups = [
        [CORES * chip_at(place) + core for place in range(devices // CORES)]
        for core in range(CORES)
    ]
    got = lax.all_to_all(
        pack(field, index), TM, 0, 0, axis_index_groups=groups, tiled=True
    )
    total_days = 1.0 * index.shape[0] * devices
    swap = [(i, i ^ 1) for i in range(devices)]
    return after(
        got, lag_list, index_offset, sea_mask, total_days, lambda x: lax.ppermute(x, TM, swap)
    )


def solution(mesh):
    return jax.shard_map(
        shards,
        mesh=mesh,
        in_specs=(P(TM, None), P(TM, None), P(), P(), P(TM)),
        out_specs=P(TM, None, None),
        check_vma=False,
    )
```

```python
import jax
import jax.numpy as jnp
from jax import lax
from jax.experimental import pallas as pl
from jax.experimental.pallas import tpu as pltpu
from jax.sharding import PartitionSpec as P

TM = "tm"
CORES = 2
WEIGHTS = (1, 16, 4)
DIGITS = ((3, 2, 1, 0), (3, 2, 1, 0), (2, 3, 0, 1))
PHASES = 6
KCOUNT = 10
USED = PHASES * KCOUNT
LANES = 128
HALF = 64
BEFORE = 8
TILES = 7
WIDTH = TILES * LANES
SUM_LANE = BEFORE * HALF + USED
SQUARE_LANE = SUM_LANE + 1
ROWS = HALF + 16
STEP = 8
EARLY = 32
F32 = jnp.float32
BF16 = jnp.bfloat16
VMEM = pl.BlockSpec(memory_space=pltpu.VMEM)
ANY = pl.BlockSpec(memory_space=pl.ANY)
SMALL = pltpu.CompilerParams(vmem_limit_bytes=8 << 20)


def chip_at(place):
    chip = 0
    for i, (weight, digits) in enumerate(zip(WEIGHTS, DIGITS)):
        digit = (place >> (4 - 2 * i)) & 3
        table = sum(value << (2 * at) for at, value in enumerate(digits))
        chip = chip + weight * ((table >> (2 * digit)) & 3)
    return chip


def local(array):
    return pltpu.with_memory_space_constraint(array, pltpu.VMEM)


def fill_order(early, late):
    for target in (early, late):
        days = target.shape[0]
        length = days // PHASES
        row = lax.broadcasted_iota(jnp.int32, (length, days), 0)
        column = lax.broadcasted_iota(jnp.int32, (length, days), 1)
        for r in range(PHASES):
            target[r * length : (r + 1) * length, :] = (column == row * PHASES + r).astype(BF16)


def order_scratch(t_dev):
    ahead = EARLY * PHASES
    return [pltpu.VMEM((ahead, ahead), BF16), pltpu.VMEM((t_dev - ahead, t_dev - ahead), BF16)]


def pack_kernel(field_ref, index_ref, sent_ref, index, early, late, sems, index_sem):
    kcount, t_dev = index_ref.shape
    count = t_dev // PHASES
    chips = sent_ref.shape[0]
    ahead = EARLY * PHASES
    index_copy = pltpu.make_async_copy(index_ref, index, index_sem)
    index_copy.start()

    def copy(place):
        lanes = pl.ds(pl.multiple_of(chip_at(place) * LANES, LANES), LANES)
        return pltpu.make_async_copy(
            field_ref.at[:, lanes], sent_ref.at[place, 0:t_dev, :], sems.at[place]
        )

    def start(place, _):
        copy(place).start()
        return 0

    lax.fori_loop(0, chips, start, 0, unroll=8)
    fill_order(early, late)
    index_copy.wait()
    rest = index[...]
    gap = jnp.zeros((16 - kcount, 1), F32)
    rest_sums = jnp.concatenate(
        [
            jnp.sum(rest, 1, keepdims=True),
            gap,
            jnp.sum(rest * rest, 1, keepdims=True),
            jnp.zeros((count - 16 - kcount, 1), F32),
        ],
        0,
    )
    spare = []
    for _ in range(3):
        spare.append(rest_sums.astype(BF16).astype(F32))
        rest_sums = rest_sums - spare[-1]
    spare.append(jnp.zeros((count, 1), F32))
    value = jnp.zeros((count, USED), F32)
    for _ in range(3):
        part = rest.astype(BF16)
        rest = rest - part.astype(F32)
        first = lax.dot_general(
            early[...], part[:, :ahead], (((1,), (1,)), ((), ())), preferred_element_type=F32
        )
        second = lax.dot_general(
            late[...], part[:, ahead:], (((1,), (1,)), ((), ())), preferred_element_type=F32
        )
        later = count - EARLY
        value = value + jnp.concatenate(
            [
                jnp.concatenate(
                    [first[r * EARLY : (r + 1) * EARLY], second[r * later : (r + 1) * later]], 0
                )
                for r in range(PHASES)
            ],
            1,
        )
    origin = value[0:1].astype(BF16).astype(F32)
    top = lax.broadcasted_iota(jnp.int32, value.shape, 0) == 0
    value = jnp.where(top, value, value - origin)
    upper = value.astype(BF16).astype(F32)
    blank = jnp.zeros((count, HALF - USED), F32)
    rows = jnp.concatenate([upper] + spare + [value - upper, blank], 1).astype(BF16)

    def repeat(place, _):
        sent_ref[place, t_dev:, :] = rows
        return 0

    lax.fori_loop(0, chips, repeat, 0, unroll=8)

    def finish_copy(place, _):
        copy(place).wait()
        return 0

    lax.fori_loop(0, chips, finish_copy, 0, unroll=8)


def pack(field, index):
    t_dev, cells = field.shape
    chips = cells // LANES
    return pl.pallas_call(
        pack_kernel,
        in_specs=[ANY] * 2,
        out_specs=VMEM,
        out_shape=pltpu.VMEM((chips, t_dev + t_dev // PHASES, LANES), BF16),
        scratch_shapes=[pltpu.VMEM(index.T.shape, F32)]
        + order_scratch(t_dev)
        + [pltpu.SemaphoreType.DMA((chips,)), pltpu.SemaphoreType.DMA],
        compiler_params=SMALL,
    )(*[pltpu.with_memory_space_constraint(x, pltpu.HBM) for x in (field, index.T)])


def joined(raw):
    wide = raw.astype(F32)
    turned = pltpu.roll(wide, HALF, 1)
    value = wide + turned
    lane = lax.broadcasted_iota(jnp.int32, (1, LANES), 1)
    origin = jnp.where(lane < HALF, wide[0:1], turned[0:1])
    top = lax.broadcasted_iota(jnp.int32, value.shape, 0) == 0
    return jnp.where(top, value, value + origin)


def summed(value):
    return jnp.sum(value.reshape(-1, 8, LANES), 0)


def take_kernel(got_ref, edge_ref):
    chips, rows, _ = got_ref.shape
    count = rows // (PHASES + 1)
    start = rows - count
    lane = lax.broadcasted_iota(jnp.int32, (1, LANES), 1)
    top = lax.broadcasted_iota(jnp.int32, (8, LANES), 0) == 0

    def body(place, sums):
        head = got_ref[place, start : start + 32, :].astype(F32)
        tail = got_ref[place, rows - 8 :, :].astype(F32)
        turned = pltpu.roll(head[0:8], HALF, 1)
        origin = jnp.where(lane < HALF, head[0:1], turned[0:1])
        value = head[0:8] + turned
        chip = chip_at(place)
        edge_ref[chip, 0:8, :] = jnp.where(top, value, value + origin)
        edge_ref[chip, 8:16, :] = tail + pltpu.roll(tail, HALF, 1) + origin
        return sums + head

    sums = lax.fori_loop(0, chips, body, jnp.zeros((32, LANES), F32), unroll=64)
    spare = (lane >= USED) & (lane < HALF)
    sums = jnp.sum(jnp.where(spare, sums, 0.0), 1, keepdims=True)
    edge_ref[chips] = jnp.where(lane == 0, sums[0:16], jnp.where(lane == 1, sums[16:32], 0.0))


def take_index(got):
    return pl.pallas_call(
        take_kernel,
        in_specs=[VMEM],
        out_specs=VMEM,
        out_shape=pltpu.VMEM((got.shape[0] + 1, 16, LANES), F32),
        compiler_params=SMALL,
    )(local(got))


def middle_kernel(got_ref, days_ref, square_ref, early, late):
    chips, rows, _ = got_ref.shape
    t_dev = rows * PHASES // (PHASES + 1)
    count = t_dev // PHASES
    ahead = EARLY * PHASES
    fill_order(early, late)

    def body(pair, square):
        start = pl.multiple_of(pair * 2 * count, 16)
        for source, days, base in ((early, slice(0, ahead), 0), (late, slice(ahead, t_dev), EARLY)):
            length = source.shape[0] // PHASES
            blocks = [got_ref[2 * pair + side, days, :] for side in range(2)]
            for block in blocks:
                wide = block.astype(F32)
                square = square + jnp.sum((wide * wide).reshape(-1, 16, LANES), 0)
            mixed = jnp.dot(
                source[...], jnp.concatenate(blocks, 1), preferred_element_type=F32
            )
            for r in range(PHASES):
                piece = mixed[r * length : (r + 1) * length].astype(BF16)
                days_ref[r, pl.ds(start + base, length), :] = piece[:, :LANES]
                days_ref[r, pl.ds(start + count + base, length), :] = piece[:, LANES:]
        return square

    square_ref[...] = lax.fori_loop(0, chips // 2, body, jnp.zeros((16, LANES), F32), unroll=32)


def middle(got, t_dev):
    chips = got.shape[0]
    return pl.pallas_call(
        middle_kernel,
        in_specs=[VMEM],
        out_specs=[VMEM] * 2,
        out_shape=[
            pltpu.VMEM((PHASES, chips * t_dev // PHASES, LANES), BF16),
            pltpu.VMEM((16, LANES), F32),
        ],
        scratch_shapes=order_scratch(t_dev),
        compiler_params=SMALL,
    )(local(got))


def spread_kernel(
    got_ref, mine_ref, other_ref, square_ref, days,
    kept_ref, passed_ref, stat_ref,
    edge, line, slid, win, late_win, acc, merged,
):
    chips, rows, _ = got_ref.shape
    count = rows // (PHASES + 1)
    core = lax.rem(lax.axis_index(TM), CORES)
    total_days = 2.0 * chips * count * PHASES
    zero = jnp.zeros((8, LANES), F32)
    sums = mine_ref[chips] + other_ref[chips]
    mean = sums[:, 0:1] / total_days
    var = sums[:, 1:2] / total_days - mean * mean
    row = lax.broadcasted_iota(jnp.int32, (16, LANES), 0)
    column = lax.broadcasted_iota(jnp.int32, (16, LANES), 1) % HALF
    same = (column < USED) & (column % KCOUNT == row)
    mean = jnp.sum(jnp.where(same, mean, 0.0), 0, keepdims=True)
    var = jnp.sum(jnp.where(same, var, 0.0), 0, keepdims=True)
    stat_ref[...] = jnp.concatenate([mean, var, jnp.zeros((6, LANES), F32)], 0)
    lane = lax.broadcasted_iota(jnp.int32, (1, LANES), 1)
    valid = lane % HALF < USED

    def centered(value):
        return jnp.where(valid, (value - mean).astype(BF16).astype(F32), 0.0)

    edge[0] = jnp.broadcast_to(mean, (16, LANES))
    edge[chips + 1] = jnp.broadcast_to(mean, (16, LANES))

    def move(chip, _):
        edge[chip + 1] = other_ref[chip]
        return 0

    lax.fori_loop(0, chips, move, 0, unroll=16)

    def slide(group, sums, target, offset, base):
        sums = list(sums)
        for side in range(8):
            place = 8 * group + side
            chip = chip_at(place)
            at = base + side
            line[at, 0:8, :] = centered(edge[chip + core, 8:16, :])
            line[at, 8 : 8 + count, :] = jnp.where(lane == USED, 1.0, centered(joined(got_ref[place, rows - count :, :])))
            line[at, 8 + count :, :] = centered(edge[chip + core + 1, 0:8, :])
            sums[0] = sums[0] + line[at, 0:16, :] - line[at, count : count + 16, :]
            sums[1] = sums[1] + summed(line[at, 8 : 8 + count, :])
        for side in range(8):
            at = base + side
            slid[at, 0 : count + 15, :] = jnp.where(
                lane < HALF, line[at, 0 : count + 15, :], line[at, 1 : count + 16, :]
            )
        start = (8 * group - offset) * count
        if not isinstance(start, int):
            start = pl.multiple_of(start, 16)
        for pair in range(8 // 2):
            for q in range(TILES):
                tile = jnp.concatenate(
                    [slid[base + 2 * pair + side, 2 * q : 2 * q + count, :] for side in range(2)], 0
                )
                target[q, pl.ds(start + pair * 2 * count, 2 * count), :] = tile.astype(BF16)
        return tuple(sums)

    def multiply(source, rows):
        return lax.dot_general(
            jnp.concatenate([source[q] for q in range(TILES)], 1),
            jnp.concatenate([days[r, rows, :] for r in range(PHASES)], 1),
            (((0,), (0,)), ((), ())),
            preferred_element_type=F32,
        )

    half = chips // 2
    window_sums = lax.fori_loop(
        0, half // 8, lambda g, sums: slide(g, sums, win, 0, 0), (jnp.zeros((16, LANES), F32), zero),
        unroll=True,
    )
    acc[0:WIDTH, :] = multiply(win, slice(0, half * count))
    for group in range(half // 8, chips // 8):
        window_sums = slide(group, window_sums, late_win, half, 8 * (group % 2))
    acc[0:WIDTH, :] += multiply(late_win, slice(half * count, chips * count))
    edges, inner = window_sums
    acc[WIDTH:, :] = jnp.zeros((HALF, PHASES * LANES), F32)
    inner = jnp.sum(inner, 0, keepdims=True)
    at = lax.broadcasted_iota(jnp.int32, (16, LANES), 0)
    upper_half = (lax.broadcasted_iota(jnp.int32, (16, LANES), 1) >= HALF).astype(jnp.int32)
    window_sums = []
    for q in range(TILES):
        move = 2 * q - BEFORE + upper_half
        gained = (at >= 8 + move) & (at < 8)
        lost = (at >= 8) & (at < 8 + move)
        change = jnp.where(gained, edges, 0.0) - jnp.where(lost, edges, 0.0)
        window_sums.append(inner + jnp.sum(change, 0, keepdims=True))
    sums_row = jnp.concatenate(window_sums, 1)

    def shifted(parts):
        total = parts[0]
        lanes = lax.broadcasted_iota(jnp.int32, total.shape, 1) % HALF
        for r in range(1, PHASES):
            near = pltpu.roll(parts[r], WIDTH - KCOUNT * r, 1)
            far = pltpu.roll(parts[r], WIDTH - KCOUNT * r - (HALF - USED), 1)
            total = total + jnp.where(lanes + KCOUNT * r < USED, near, far)
        return total

    squared = jnp.sum(square_ref[...], 0, keepdims=True)
    inside = lax.broadcasted_iota(jnp.int32, (LANES, LANES), 0) % HALF
    for tile in range(TILES):
        base = tile * LANES
        total = acc[base : base + LANES, 0:LANES]
        for r in range(1, PHASES):
            lanes = slice(r * LANES, (r + 1) * LANES)
            near = base + KCOUNT * r
            far = near + HALF - USED
            total = total + jnp.where(
                inside + KCOUNT * r < USED,
                acc[near : near + LANES, lanes],
                acc[far : far + LANES, lanes],
            )
        if base <= SUM_LANE < base + LANES:
            at = lax.broadcasted_iota(jnp.int32, (LANES, LANES), 0) + base
            plain = sum(acc[base : base + LANES, r * LANES : (r + 1) * LANES] for r in range(PHASES))
            total = jnp.where(at == SUM_LANE, plain, total)
            total = jnp.where(at == SQUARE_LANE, squared, total)
        merged[:, base : base + LANES] = jnp.transpose(total)
    totals = shifted([jnp.broadcast_to(sums_row, (8, WIDTH))] * PHASES)
    kept_ref[0:HALF, :] = merged[pl.ds(pl.multiple_of(core * HALF, HALF), HALF), :]
    passed_ref[0:HALF, :] = merged[pl.ds(pl.multiple_of((1 - core) * HALF, HALF), HALF), :]
    for target in (kept_ref, passed_ref):
        target[HALF : HALF + 8, :] = totals
        target[HALF + 8 :, :] = totals


def spread(got, mine, other, square, days):
    chips, rows, _ = got.shape
    count = rows // (PHASES + 1)
    return pl.pallas_call(
        spread_kernel,
        in_specs=[VMEM] * 5,
        out_specs=[VMEM] * 3,
        out_shape=[
            pltpu.VMEM((ROWS, WIDTH), F32),
            pltpu.VMEM((ROWS, WIDTH), F32),
            pltpu.VMEM((8, LANES), F32),
        ],
        scratch_shapes=[
            pltpu.VMEM((chips + 2, 16, LANES), F32),
            pltpu.VMEM((16, count + 16, LANES), F32),
            pltpu.VMEM((16, count + 16, LANES), F32),
            pltpu.VMEM((TILES, chips * count // 2, LANES), BF16),
            pltpu.VMEM((TILES, chips * count // 2, LANES), BF16),
            pltpu.VMEM((WIDTH + HALF, PHASES * LANES), F32),
            pltpu.VMEM((LANES, WIDTH), F32),
        ],
        compiler_params=pltpu.CompilerParams(vmem_limit_bytes=32 << 20),
    )(local(got), local(mine), local(other), local(square), local(days))


def finish_kernel(
    kept_ref, taken_ref, stat_ref, lag_ref, mask_ref, offset_ref, out_ref,
    base, maps, sems, *, total_days,
):
    slots = lax.broadcasted_iota(jnp.int32, (WIDTH + 16, LANES), 0) - 16
    slot = lax.broadcasted_iota(jnp.int32, (1, LANES), 1)
    group = lax.shift_right_logical(slot * 43, 8)
    place = jnp.where(slot < TILES * 2 * PHASES, HALF * group + KCOUNT * (slot - PHASES * group), -100)
    base[...] = (slots == place).astype(F32)
    value = kept_ref[...] + taken_ref[...]
    upper = value.astype(BF16)
    rest = value - upper.astype(F32)
    middle = rest.astype(BF16)
    lower = (rest - middle.astype(F32)).astype(BF16)
    mean_x = value[0:HALF, SUM_LANE : SUM_LANE + 1] / total_days
    var_x = value[0:HALF, SQUARE_LANE : SQUARE_LANE + 1] / total_days - mean_x * mean_x
    scale_x = total_days * jnp.sqrt(var_x + 1e-06)
    scale_i = jnp.sqrt(stat_ref[1:2, :] + 1e-06)
    mask = jnp.concatenate([mask_ref[...].astype(F32), jnp.zeros((1, LANES - HALF), F32)], 1)
    mask = jnp.transpose(jnp.broadcast_to(mask, (LANES, LANES)))[0:HALF, 0:1]
    lags = lag_ref.shape[1]
    lag = jnp.concatenate([lag_ref[...], jnp.zeros((1, LANES - lags), jnp.int32)], 1)
    parts = jnp.concatenate([upper, middle, lower], 0)
    copies = []
    for pair in range(KCOUNT // 2):
        picker = jnp.concatenate(
            [base[16 - k : 16 - k + WIDTH, :].astype(BF16) for k in (2 * pair, 2 * pair + 1)], 1
        )
        thirds = jnp.dot(parts, picker, preferred_element_type=F32)
        chosen = thirds[0:ROWS] + thirds[ROWS : 2 * ROWS] + thirds[2 * ROWS :]
        for side in range(2):
            k = 2 * pair + side
            part = chosen[:, side * LANES : (side + 1) * LANES]
            wanted = BEFORE * PHASES - (lag + offset_ref[:, k : k + 1])
            part = jnp.take_along_axis(
                part, jnp.broadcast_to(wanted, part.shape), axis=1, mode="promise_in_bounds"
            )
            numer = part[0:HALF] - mean_x * part[HALF : HALF + 1]
            answer = numer / (scale_x * scale_i[:, k : k + 1]) * mask
            maps[k] = answer[:, :lags]
        copy = pltpu.make_async_copy(
            maps.at[2 * pair : 2 * pair + 2], out_ref.at[2 * pair : 2 * pair + 2], sems.at[pair]
        )
        copy.start()
        copies.append(copy)
    for copy in copies:
        copy.wait()


def finish(kept, taken, stat, lag_list, index_offset, mask, total_days):
    lags = lag_list.shape[0]
    return pl.pallas_call(
        lambda *refs: finish_kernel(*refs, total_days=total_days),
        in_specs=[VMEM] * 6,
        out_specs=ANY,
        out_shape=pltpu.HBM((KCOUNT, HALF, lags), F32),
        scratch_shapes=[
            pltpu.VMEM((WIDTH + 16, LANES), F32),
            pltpu.VMEM((KCOUNT, HALF, lags), F32),
            pltpu.SemaphoreType.DMA((KCOUNT // 2,)),
        ],
        compiler_params=SMALL,
    )(
        local(kept), local(taken), local(stat), local(lag_list[None, :]), local(mask[None, :]),
        local(index_offset[None, :]),
    )


def after(got, lag_list, index_offset, sea_mask, total_days, swapped):
    t_dev = got.shape[1] * PHASES // (PHASES + 1)
    mine = take_index(got)
    other = swapped(mine)
    days, square = middle(got, t_dev)
    kept, passed, stat = spread(got, mine, other, square, days)
    taken = swapped(passed)
    maps = finish(kept, taken, stat, lag_list, index_offset, sea_mask, total_days)
    return jnp.transpose(maps, (1, 0, 2))


def shards(field, index, lag_list, index_offset, sea_mask):
    devices = lax.axis_size(TM)
    groups = [
        [CORES * chip_at(place) + core for place in range(devices // CORES)]
        for core in range(CORES)
    ]
    got = lax.all_to_all(
        pack(field, index), TM, 0, 0, axis_index_groups=groups, tiled=True
    )
    total_days = 1.0 * index.shape[0] * devices
    swap = [(i, i ^ 1) for i in range(devices)]
    return after(
        got, lag_list, index_offset, sea_mask, total_days, lambda x: lax.ppermute(x, TM, swap)
    )


def solution(mesh):
    return jax.shard_map(
        shards,
        mesh=mesh,
        in_specs=(P(TM, None), P(TM, None), P(), P(), P(TM)),
        out_specs=P(TM, None, None),
        check_vma=False,
    )
```

```python
import jax
import jax.numpy as jnp
from jax import lax
from jax.experimental import pallas as pl
from jax.experimental.pallas import tpu as pltpu
from jax.sharding import PartitionSpec as P

TM = "tm"
CORES = 2
WEIGHTS = (1, 16, 4)
DIGITS = ((3, 2, 1, 0), (3, 2, 1, 0), (2, 3, 0, 1))
PHASES = 6
KCOUNT = 10
USED = PHASES * KCOUNT
LANES = 128
HALF = 64
BEFORE = 8
TILES = 7
WIDTH = TILES * LANES
SUM_LANE = BEFORE * HALF + USED
SQUARE_LANE = SUM_LANE + 1
ROWS = HALF + 16
STEP = 8
EARLY = 32
F32 = jnp.float32
BF16 = jnp.bfloat16
VMEM = pl.BlockSpec(memory_space=pltpu.VMEM)
ANY = pl.BlockSpec(memory_space=pl.ANY)
SMALL = pltpu.CompilerParams(vmem_limit_bytes=8 << 20)


def chip_at(place):
    chip = 0
    for i, (weight, digits) in enumerate(zip(WEIGHTS, DIGITS)):
        digit = (place >> (4 - 2 * i)) & 3
        table = sum(value << (2 * at) for at, value in enumerate(digits))
        chip = chip + weight * ((table >> (2 * digit)) & 3)
    return chip


def local(array):
    return pltpu.with_memory_space_constraint(array, pltpu.VMEM)


def fill_order(early, late):
    for target in (early, late):
        days = target.shape[0]
        length = days // PHASES
        row = lax.broadcasted_iota(jnp.int32, (length, days), 0)
        column = lax.broadcasted_iota(jnp.int32, (length, days), 1)
        for r in range(PHASES):
            target[r * length : (r + 1) * length, :] = (column == row * PHASES + r).astype(BF16)


def order_scratch(t_dev):
    ahead = EARLY * PHASES
    return [pltpu.VMEM((ahead, ahead), BF16), pltpu.VMEM((t_dev - ahead, t_dev - ahead), BF16)]


def pack_kernel(field_ref, index_ref, sent_ref, index, early, late, sems, index_sem):
    kcount, t_dev = index_ref.shape
    count = t_dev // PHASES
    chips = sent_ref.shape[0]
    ahead = EARLY * PHASES
    index_copy = pltpu.make_async_copy(index_ref, index, index_sem)
    index_copy.start()

    def copy(place):
        lanes = pl.ds(pl.multiple_of(chip_at(place) * LANES, LANES), LANES)
        return pltpu.make_async_copy(
            field_ref.at[:, lanes], sent_ref.at[place, 0:t_dev, :], sems.at[place]
        )

    def start(place, _):
        copy(place).start()
        return 0

    lax.fori_loop(0, chips, start, 0, unroll=8)
    fill_order(early, late)
    index_copy.wait()
    rest = index[...]
    gap = jnp.zeros((16 - kcount, 1), F32)
    rest_sums = jnp.concatenate(
        [
            jnp.sum(rest, 1, keepdims=True),
            gap,
            jnp.sum(rest * rest, 1, keepdims=True),
            jnp.zeros((count - 16 - kcount, 1), F32),
        ],
        0,
    )
    spare = []
    for _ in range(3):
        spare.append(rest_sums.astype(BF16).astype(F32))
        rest_sums = rest_sums - spare[-1]
    spare.append(jnp.zeros((count, 1), F32))
    value = jnp.zeros((count, USED), F32)
    for _ in range(3):
        part = rest.astype(BF16)
        rest = rest - part.astype(F32)
        first = lax.dot_general(
            early[...], part[:, :ahead], (((1,), (1,)), ((), ())), preferred_element_type=F32
        )
        second = lax.dot_general(
            late[...], part[:, ahead:], (((1,), (1,)), ((), ())), preferred_element_type=F32
        )
        later = count - EARLY
        value = value + jnp.concatenate(
            [
                jnp.concatenate(
                    [first[r * EARLY : (r + 1) * EARLY], second[r * later : (r + 1) * later]], 0
                )
                for r in range(PHASES)
            ],
            1,
        )
    origin = value[0:1].astype(BF16).astype(F32)
    top = lax.broadcasted_iota(jnp.int32, value.shape, 0) == 0
    value = jnp.where(top, value, value - origin)
    upper = value.astype(BF16).astype(F32)
    blank = jnp.zeros((count, HALF - USED), F32)
    rows = jnp.concatenate([upper] + spare + [value - upper, blank], 1).astype(BF16)

    def repeat(place, _):
        sent_ref[place, t_dev:, :] = rows
        return 0

    lax.fori_loop(0, chips, repeat, 0, unroll=8)

    def finish_copy(place, _):
        copy(place).wait()
        return 0

    lax.fori_loop(0, chips, finish_copy, 0, unroll=8)


def pack(field, index):
    t_dev, cells = field.shape
    chips = cells // LANES
    return pl.pallas_call(
        pack_kernel,
        in_specs=[ANY] * 2,
        out_specs=VMEM,
        out_shape=pltpu.VMEM((chips, t_dev + t_dev // PHASES, LANES), BF16),
        scratch_shapes=[pltpu.VMEM(index.T.shape, F32)]
        + order_scratch(t_dev)
        + [pltpu.SemaphoreType.DMA((chips,)), pltpu.SemaphoreType.DMA],
        compiler_params=SMALL,
    )(*[pltpu.with_memory_space_constraint(x, pltpu.HBM) for x in (field, index.T)])


def joined(raw):
    wide = raw.astype(F32)
    turned = pltpu.roll(wide, HALF, 1)
    value = wide + turned
    lane = lax.broadcasted_iota(jnp.int32, (1, LANES), 1)
    origin = jnp.where(lane < HALF, wide[0:1], turned[0:1])
    top = lax.broadcasted_iota(jnp.int32, value.shape, 0) == 0
    return jnp.where(top, value, value + origin)


def summed(value):
    return jnp.sum(value.reshape(-1, 8, LANES), 0)


def take_kernel(got_ref, edge_ref):
    chips, rows, _ = got_ref.shape
    count = rows // (PHASES + 1)
    start = rows - count
    lane = lax.broadcasted_iota(jnp.int32, (1, LANES), 1)
    top = lax.broadcasted_iota(jnp.int32, (8, LANES), 0) == 0

    def body(place, sums):
        head = got_ref[place, start : start + 32, :].astype(F32)
        tail = got_ref[place, rows - 8 :, :].astype(F32)
        turned = pltpu.roll(head[0:8], HALF, 1)
        origin = jnp.where(lane < HALF, head[0:1], turned[0:1])
        value = head[0:8] + turned
        chip = chip_at(place)
        edge_ref[chip, 0:8, :] = jnp.where(top, value, value + origin)
        edge_ref[chip, 8:16, :] = tail + pltpu.roll(tail, HALF, 1) + origin
        return sums + head

    sums = lax.fori_loop(0, chips, body, jnp.zeros((32, LANES), F32), unroll=64)
    spare = (lane >= USED) & (lane < HALF)
    sums = jnp.sum(jnp.where(spare, sums, 0.0), 1, keepdims=True)
    edge_ref[chips] = jnp.where(lane == 0, sums[0:16], jnp.where(lane == 1, sums[16:32], 0.0))


def take_index(got):
    return pl.pallas_call(
        take_kernel,
        in_specs=[VMEM],
        out_specs=VMEM,
        out_shape=pltpu.VMEM((got.shape[0] + 1, 16, LANES), F32),
        compiler_params=SMALL,
    )(local(got))


def middle_kernel(got_ref, days_ref, square_ref, early, late):
    chips, rows, _ = got_ref.shape
    t_dev = rows * PHASES // (PHASES + 1)
    count = t_dev // PHASES
    ahead = EARLY * PHASES
    fill_order(early, late)

    def body(pair, square):
        start = pl.multiple_of(pair * 2 * count, 16)
        for source, days, base in ((early, slice(0, ahead), 0), (late, slice(ahead, t_dev), EARLY)):
            length = source.shape[0] // PHASES
            blocks = [got_ref[2 * pair + side, days, :] for side in range(2)]
            for block in blocks:
                wide = block.astype(F32)
                square = square + jnp.sum((wide * wide).reshape(-1, 16, LANES), 0)
            mixed = jnp.dot(
                source[...], jnp.concatenate(blocks, 1), preferred_element_type=F32
            )
            for r in range(PHASES):
                piece = mixed[r * length : (r + 1) * length].astype(BF16)
                days_ref[r, pl.ds(start + base, length), :] = piece[:, :LANES]
                days_ref[r, pl.ds(start + count + base, length), :] = piece[:, LANES:]
        return square

    square_ref[...] = lax.fori_loop(0, chips // 2, body, jnp.zeros((16, LANES), F32), unroll=32)


def middle(got, t_dev):
    chips = got.shape[0]
    return pl.pallas_call(
        middle_kernel,
        in_specs=[VMEM],
        out_specs=[VMEM] * 2,
        out_shape=[
            pltpu.VMEM((PHASES, chips * t_dev // PHASES, LANES), BF16),
            pltpu.VMEM((16, LANES), F32),
        ],
        scratch_shapes=order_scratch(t_dev),
        compiler_params=SMALL,
    )(local(got))


def spread_kernel(
    got_ref, mine_ref, other_ref, square_ref, days,
    kept_ref, passed_ref, stat_ref,
    edge, line, slid, win, late_win, acc, merged,
):
    chips, rows, _ = got_ref.shape
    count = rows // (PHASES + 1)
    core = lax.rem(lax.axis_index(TM), CORES)
    total_days = 2.0 * chips * count * PHASES
    zero = jnp.zeros((8, LANES), F32)
    sums = mine_ref[chips] + other_ref[chips]
    mean = sums[:, 0:1] / total_days
    var = sums[:, 1:2] / total_days - mean * mean
    row = lax.broadcasted_iota(jnp.int32, (16, LANES), 0)
    column = lax.broadcasted_iota(jnp.int32, (16, LANES), 1) % HALF
    same = (column < USED) & (column % KCOUNT == row)
    mean = jnp.sum(jnp.where(same, mean, 0.0), 0, keepdims=True)
    var = jnp.sum(jnp.where(same, var, 0.0), 0, keepdims=True)
    stat_ref[...] = jnp.concatenate([mean, var, jnp.zeros((6, LANES), F32)], 0)
    lane = lax.broadcasted_iota(jnp.int32, (1, LANES), 1)
    valid = lane % HALF < USED

    def centered(value):
        return jnp.where(valid, (value - mean).astype(BF16).astype(F32), 0.0)

    edge[0] = jnp.broadcast_to(mean, (16, LANES))
    edge[chips + 1] = jnp.broadcast_to(mean, (16, LANES))

    def move(chip, _):
        edge[chip + 1] = other_ref[chip]
        return 0

    lax.fori_loop(0, chips, move, 0, unroll=64)

    def slide(group, sums, target, offset, base):
        sums = list(sums)
        for side in range(8):
            place = 8 * group + side
            chip = chip_at(place)
            at = base + side
            line[at, 0:8, :] = centered(edge[chip + core, 8:16, :])
            line[at, 8 : 8 + count, :] = jnp.where(lane == USED, 1.0, centered(joined(got_ref[place, rows - count :, :])))
            line[at, 8 + count :, :] = centered(edge[chip + core + 1, 0:8, :])
            sums[0] = sums[0] + line[at, 0:16, :] - line[at, count : count + 16, :]
            sums[1] = sums[1] + summed(line[at, 8 : 8 + count, :])
        for side in range(8):
            at = base + side
            slid[at, 0 : count + 15, :] = jnp.where(
                lane < HALF, line[at, 0 : count + 15, :], line[at, 1 : count + 16, :]
            )
        start = (8 * group - offset) * count
        if not isinstance(start, int):
            start = pl.multiple_of(start, 16)
        for pair in range(8 // 2):
            for q in range(TILES):
                tile = jnp.concatenate(
                    [slid[base + 2 * pair + side, 2 * q : 2 * q + count, :] for side in range(2)], 0
                )
                target[q, pl.ds(start + pair * 2 * count, 2 * count), :] = tile.astype(BF16)
        return tuple(sums)

    def multiply(source, rows):
        return lax.dot_general(
            jnp.concatenate([source[q] for q in range(TILES)], 1),
            jnp.concatenate([days[r, rows, :] for r in range(PHASES)], 1),
            (((0,), (0,)), ((), ())),
            preferred_element_type=F32,
        )

    half = chips // 2
    window_sums = lax.fori_loop(
        0, half // 8, lambda g, sums: slide(g, sums, win, 0, 0), (jnp.zeros((16, LANES), F32), zero),
        unroll=True,
    )
    for group in range(half // 8, chips // 8):
        window_sums = slide(group, window_sums, late_win, half, 8 * (group % 2))
    acc[0:WIDTH, :] = multiply(win, slice(0, half * count))
    acc[0:WIDTH, :] += multiply(late_win, slice(half * count, chips * count))
    edges, inner = window_sums
    acc[WIDTH:, :] = jnp.zeros((HALF, PHASES * LANES), F32)
    inner = jnp.sum(inner, 0, keepdims=True)
    at = lax.broadcasted_iota(jnp.int32, (16, LANES), 0)
    upper_half = (lax.broadcasted_iota(jnp.int32, (16, LANES), 1) >= HALF).astype(jnp.int32)
    window_sums = []
    for q in range(TILES):
        move = 2 * q - BEFORE + upper_half
        gained = (at >= 8 + move) & (at < 8)
        lost = (at >= 8) & (at < 8 + move)
        change = jnp.where(gained, edges, 0.0) - jnp.where(lost, edges, 0.0)
        window_sums.append(inner + jnp.sum(change, 0, keepdims=True))
    sums_row = jnp.concatenate(window_sums, 1)

    def shifted(parts):
        total = parts[0]
        lanes = lax.broadcasted_iota(jnp.int32, total.shape, 1) % HALF
        for r in range(1, PHASES):
            near = pltpu.roll(parts[r], WIDTH - KCOUNT * r, 1)
            far = pltpu.roll(parts[r], WIDTH - KCOUNT * r - (HALF - USED), 1)
            total = total + jnp.where(lanes + KCOUNT * r < USED, near, far)
        return total

    squared = jnp.sum(square_ref[...], 0, keepdims=True)
    inside = lax.broadcasted_iota(jnp.int32, (LANES, LANES), 0) % HALF
    for tile in range(TILES):
        base = tile * LANES
        total = acc[base : base + LANES, 0:LANES]
        for r in range(1, PHASES):
            lanes = slice(r * LANES, (r + 1) * LANES)
            near = base + KCOUNT * r
            far = near + HALF - USED
            total = total + jnp.where(
                inside + KCOUNT * r < USED,
                acc[near : near + LANES, lanes],
                acc[far : far + LANES, lanes],
            )
        if base <= SUM_LANE < base + LANES:
            at = lax.broadcasted_iota(jnp.int32, (LANES, LANES), 0) + base
            plain = sum(acc[base : base + LANES, r * LANES : (r + 1) * LANES] for r in range(PHASES))
            total = jnp.where(at == SUM_LANE, plain, total)
            total = jnp.where(at == SQUARE_LANE, squared, total)
        merged[:, base : base + LANES] = jnp.transpose(total)
    totals = shifted([jnp.broadcast_to(sums_row, (8, WIDTH))] * PHASES)
    kept_ref[0:HALF, :] = merged[pl.ds(pl.multiple_of(core * HALF, HALF), HALF), :]
    passed_ref[0:HALF, :] = merged[pl.ds(pl.multiple_of((1 - core) * HALF, HALF), HALF), :]
    for target in (kept_ref, passed_ref):
        target[HALF : HALF + 8, :] = totals
        target[HALF + 8 :, :] = totals


def spread(got, mine, other, square, days):
    chips, rows, _ = got.shape
    count = rows // (PHASES + 1)
    return pl.pallas_call(
        spread_kernel,
        in_specs=[VMEM] * 5,
        out_specs=[VMEM] * 3,
        out_shape=[
            pltpu.VMEM((ROWS, WIDTH), F32),
            pltpu.VMEM((ROWS, WIDTH), F32),
            pltpu.VMEM((8, LANES), F32),
        ],
        scratch_shapes=[
            pltpu.VMEM((chips + 2, 16, LANES), F32),
            pltpu.VMEM((16, count + 16, LANES), F32),
            pltpu.VMEM((16, count + 16, LANES), F32),
            pltpu.VMEM((TILES, chips * count // 2, LANES), BF16),
            pltpu.VMEM((TILES, chips * count // 2, LANES), BF16),
            pltpu.VMEM((WIDTH + HALF, PHASES * LANES), F32),
            pltpu.VMEM((LANES, WIDTH), F32),
        ],
        compiler_params=pltpu.CompilerParams(vmem_limit_bytes=32 << 20),
    )(local(got), local(mine), local(other), local(square), local(days))


def finish_kernel(
    kept_ref, taken_ref, stat_ref, lag_ref, mask_ref, offset_ref, out_ref,
    base, maps, sems, *, total_days,
):
    slots = lax.broadcasted_iota(jnp.int32, (WIDTH + 16, LANES), 0) - 16
    slot = lax.broadcasted_iota(jnp.int32, (1, LANES), 1)
    group = lax.shift_right_logical(slot * 43, 8)
    place = jnp.where(slot < TILES * 2 * PHASES, HALF * group + KCOUNT * (slot - PHASES * group), -100)
    base[...] = (slots == place).astype(F32)
    value = kept_ref[...] + taken_ref[...]
    upper = value.astype(BF16)
    rest = value - upper.astype(F32)
    middle = rest.astype(BF16)
    lower = (rest - middle.astype(F32)).astype(BF16)
    mean_x = value[0:HALF, SUM_LANE : SUM_LANE + 1] / total_days
    var_x = value[0:HALF, SQUARE_LANE : SQUARE_LANE + 1] / total_days - mean_x * mean_x
    scale_x = total_days * jnp.sqrt(var_x + 1e-06)
    scale_i = jnp.sqrt(stat_ref[1:2, :] + 1e-06)
    mask = jnp.concatenate([mask_ref[...].astype(F32), jnp.zeros((1, LANES - HALF), F32)], 1)
    mask = jnp.transpose(jnp.broadcast_to(mask, (LANES, LANES)))[0:HALF, 0:1]
    lags = lag_ref.shape[1]
    lag = jnp.concatenate([lag_ref[...], jnp.zeros((1, LANES - lags), jnp.int32)], 1)
    parts = jnp.concatenate([upper, middle, lower], 0)
    copies = []
    for pair in range(KCOUNT // 2):
        picker = jnp.concatenate(
            [base[16 - k : 16 - k + WIDTH, :].astype(BF16) for k in (2 * pair, 2 * pair + 1)], 1
        )
        thirds = jnp.dot(parts, picker, preferred_element_type=F32)
        chosen = thirds[0:ROWS] + thirds[ROWS : 2 * ROWS] + thirds[2 * ROWS :]
        for side in range(2):
            k = 2 * pair + side
            part = chosen[:, side * LANES : (side + 1) * LANES]
            wanted = BEFORE * PHASES - (lag + offset_ref[:, k : k + 1])
            part = jnp.take_along_axis(
                part, jnp.broadcast_to(wanted, part.shape), axis=1, mode="promise_in_bounds"
            )
            numer = part[0:HALF] - mean_x * part[HALF : HALF + 1]
            answer = numer / (scale_x * scale_i[:, k : k + 1]) * mask
            maps[k] = answer[:, :lags]
        copy = pltpu.make_async_copy(
            maps.at[2 * pair : 2 * pair + 2], out_ref.at[2 * pair : 2 * pair + 2], sems.at[pair]
        )
        copy.start()
        copies.append(copy)
    for copy in copies:
        copy.wait()


def finish(kept, taken, stat, lag_list, index_offset, mask, total_days):
    lags = lag_list.shape[0]
    return pl.pallas_call(
        lambda *refs: finish_kernel(*refs, total_days=total_days),
        in_specs=[VMEM] * 6,
        out_specs=ANY,
        out_shape=pltpu.HBM((KCOUNT, HALF, lags), F32),
        scratch_shapes=[
            pltpu.VMEM((WIDTH + 16, LANES), F32),
            pltpu.VMEM((KCOUNT, HALF, lags), F32),
            pltpu.SemaphoreType.DMA((KCOUNT // 2,)),
        ],
        compiler_params=SMALL,
    )(
        local(kept), local(taken), local(stat), local(lag_list[None, :]), local(mask[None, :]),
        local(index_offset[None, :]),
    )


def after(got, lag_list, index_offset, sea_mask, total_days, swapped):
    t_dev = got.shape[1] * PHASES // (PHASES + 1)
    mine = take_index(got)
    other = swapped(mine)
    days, square = middle(got, t_dev)
    kept, passed, stat = spread(got, mine, other, square, days)
    taken = swapped(passed)
    maps = finish(kept, taken, stat, lag_list, index_offset, sea_mask, total_days)
    return jnp.transpose(maps, (1, 0, 2))


def shards(field, index, lag_list, index_offset, sea_mask):
    devices = lax.axis_size(TM)
    groups = [
        [CORES * chip_at(place) + core for place in range(devices // CORES)]
        for core in range(CORES)
    ]
    got = lax.all_to_all(
        pack(field, index), TM, 0, 0, axis_index_groups=groups, tiled=True
    )
    total_days = 1.0 * index.shape[0] * devices
    swap = [(i, i ^ 1) for i in range(devices)]
    return after(
        got, lag_list, index_offset, sea_mask, total_days, lambda x: lax.ppermute(x, TM, swap)
    )


def solution(mesh):
    return jax.shard_map(
        shards,
        mesh=mesh,
        in_specs=(P(TM, None), P(TM, None), P(), P(), P(TM)),
        out_specs=P(TM, None, None),
        check_vma=False,
    )
```

```python
import jax
import jax.numpy as jnp
from jax import lax
from jax.experimental import pallas as pl
from jax.experimental.pallas import tpu as pltpu
from jax.sharding import PartitionSpec as P

TM = "tm"
CORES = 2
WEIGHTS = (1, 16, 4)
DIGITS = ((3, 2, 1, 0), (3, 2, 1, 0), (2, 3, 0, 1))
PHASES = 6
KCOUNT = 10
USED = PHASES * KCOUNT
LANES = 128
HALF = 64
BEFORE = 8
TILES = 7
WIDTH = TILES * LANES
SUM_LANE = BEFORE * HALF + USED
SQUARE_LANE = SUM_LANE + 1
ROWS = HALF + 16
STEP = 8
EARLY = 32
F32 = jnp.float32
BF16 = jnp.bfloat16
VMEM = pl.BlockSpec(memory_space=pltpu.VMEM)
ANY = pl.BlockSpec(memory_space=pl.ANY)
SMALL = pltpu.CompilerParams(vmem_limit_bytes=8 << 20)


def chip_at(place):
    chip = 0
    for i, (weight, digits) in enumerate(zip(WEIGHTS, DIGITS)):
        digit = (place >> (4 - 2 * i)) & 3
        table = sum(value << (2 * at) for at, value in enumerate(digits))
        chip = chip + weight * ((table >> (2 * digit)) & 3)
    return chip


def local(array):
    return pltpu.with_memory_space_constraint(array, pltpu.VMEM)


def fill_order(early, late):
    for target in (early, late):
        days = target.shape[0]
        length = days // PHASES
        row = lax.broadcasted_iota(jnp.int32, (length, days), 0)
        column = lax.broadcasted_iota(jnp.int32, (length, days), 1)
        for r in range(PHASES):
            target[r * length : (r + 1) * length, :] = (column == row * PHASES + r).astype(BF16)


def order_scratch(t_dev):
    ahead = EARLY * PHASES
    return [pltpu.VMEM((ahead, ahead), BF16), pltpu.VMEM((t_dev - ahead, t_dev - ahead), BF16)]


def pack_kernel(field_ref, index_ref, sent_ref, index, early, late, sems, index_sem):
    kcount, t_dev = index_ref.shape
    count = t_dev // PHASES
    chips = sent_ref.shape[0]
    ahead = EARLY * PHASES
    index_copy = pltpu.make_async_copy(index_ref, index, index_sem)
    index_copy.start()

    def copy(place):
        lanes = pl.ds(pl.multiple_of(chip_at(place) * LANES, LANES), LANES)
        return pltpu.make_async_copy(
            field_ref.at[:, lanes], sent_ref.at[place, 0:t_dev, :], sems.at[place]
        )

    def start(place, _):
        copy(place).start()
        return 0

    lax.fori_loop(0, chips, start, 0, unroll=8)
    fill_order(early, late)
    index_copy.wait()
    rest = index[...]
    gap = jnp.zeros((16 - kcount, 1), F32)
    rest_sums = jnp.concatenate(
        [
            jnp.sum(rest, 1, keepdims=True),
            gap,
            jnp.sum(rest * rest, 1, keepdims=True),
            jnp.zeros((count - 16 - kcount, 1), F32),
        ],
        0,
    )
    spare = []
    for _ in range(3):
        spare.append(rest_sums.astype(BF16).astype(F32))
        rest_sums = rest_sums - spare[-1]
    spare.append(jnp.zeros((count, 1), F32))
    value = jnp.zeros((count, USED), F32)
    for _ in range(3):
        part = rest.astype(BF16)
        rest = rest - part.astype(F32)
        first = lax.dot_general(
            early[...], part[:, :ahead], (((1,), (1,)), ((), ())), preferred_element_type=F32
        )
        second = lax.dot_general(
            late[...], part[:, ahead:], (((1,), (1,)), ((), ())), preferred_element_type=F32
        )
        later = count - EARLY
        value = value + jnp.concatenate(
            [
                jnp.concatenate(
                    [first[r * EARLY : (r + 1) * EARLY], second[r * later : (r + 1) * later]], 0
                )
                for r in range(PHASES)
            ],
            1,
        )
    origin = value[0:1].astype(BF16).astype(F32)
    top = lax.broadcasted_iota(jnp.int32, value.shape, 0) == 0
    value = jnp.where(top, value, value - origin)
    upper = value.astype(BF16).astype(F32)
    blank = jnp.zeros((count, HALF - USED), F32)
    rows = jnp.concatenate([upper] + spare + [value - upper, blank], 1).astype(BF16)

    def repeat(place, _):
        sent_ref[place, t_dev:, :] = rows
        return 0

    lax.fori_loop(0, chips, repeat, 0, unroll=8)

    def finish_copy(place, _):
        copy(place).wait()
        return 0

    lax.fori_loop(0, chips, finish_copy, 0, unroll=8)


def pack(field, index):
    t_dev, cells = field.shape
    chips = cells // LANES
    return pl.pallas_call(
        pack_kernel,
        in_specs=[ANY] * 2,
        out_specs=VMEM,
        out_shape=pltpu.VMEM((chips, t_dev + t_dev // PHASES, LANES), BF16),
        scratch_shapes=[pltpu.VMEM(index.T.shape, F32)]
        + order_scratch(t_dev)
        + [pltpu.SemaphoreType.DMA((chips,)), pltpu.SemaphoreType.DMA],
        compiler_params=SMALL,
    )(*[pltpu.with_memory_space_constraint(x, pltpu.HBM) for x in (field, index.T)])


def joined(raw):
    wide = raw.astype(F32)
    turned = pltpu.roll(wide, HALF, 1)
    value = wide + turned
    lane = lax.broadcasted_iota(jnp.int32, (1, LANES), 1)
    origin = jnp.where(lane < HALF, wide[0:1], turned[0:1])
    top = lax.broadcasted_iota(jnp.int32, value.shape, 0) == 0
    return jnp.where(top, value, value + origin)


def summed(value):
    return jnp.sum(value.reshape(-1, 8, LANES), 0)


def take_kernel(got_ref, edge_ref):
    chips, rows, _ = got_ref.shape
    count = rows // (PHASES + 1)
    start = rows - count
    lane = lax.broadcasted_iota(jnp.int32, (1, LANES), 1)
    top = lax.broadcasted_iota(jnp.int32, (8, LANES), 0) == 0

    def body(place, sums):
        head = got_ref[place, start : start + 32, :].astype(F32)
        tail = got_ref[place, rows - 8 :, :].astype(F32)
        turned = pltpu.roll(head[0:8], HALF, 1)
        origin = jnp.where(lane < HALF, head[0:1], turned[0:1])
        value = head[0:8] + turned
        chip = chip_at(place)
        edge_ref[chip, 0:8, :] = jnp.where(top, value, value + origin)
        edge_ref[chip, 8:16, :] = tail + pltpu.roll(tail, HALF, 1) + origin
        return sums + head

    sums = lax.fori_loop(0, chips, body, jnp.zeros((32, LANES), F32), unroll=64)
    spare = (lane >= USED) & (lane < HALF)
    sums = jnp.sum(jnp.where(spare, sums, 0.0), 1, keepdims=True)
    edge_ref[chips] = jnp.where(lane == 0, sums[0:16], jnp.where(lane == 1, sums[16:32], 0.0))


def take_index(got):
    return pl.pallas_call(
        take_kernel,
        in_specs=[VMEM],
        out_specs=VMEM,
        out_shape=pltpu.VMEM((got.shape[0] + 1, 16, LANES), F32),
        compiler_params=SMALL,
    )(local(got))


def middle_kernel(got_ref, days_ref, square_ref, early, late):
    chips, rows, _ = got_ref.shape
    t_dev = rows * PHASES // (PHASES + 1)
    count = t_dev // PHASES
    ahead = EARLY * PHASES
    fill_order(early, late)

    def body(pair, square):
        start = pl.multiple_of(pair * 2 * count, 16)
        for source, days, base in ((early, slice(0, ahead), 0), (late, slice(ahead, t_dev), EARLY)):
            length = source.shape[0] // PHASES
            blocks = [got_ref[2 * pair + side, days, :] for side in range(2)]
            for block in blocks:
                wide = block.astype(F32)
                square = square + jnp.sum((wide * wide).reshape(-1, 16, LANES), 0)
            mixed = jnp.dot(
                source[...], jnp.concatenate(blocks, 1), preferred_element_type=F32
            )
            for r in range(PHASES):
                piece = mixed[r * length : (r + 1) * length].astype(BF16)
                days_ref[r, pl.ds(start + base, length), :] = piece[:, :LANES]
                days_ref[r, pl.ds(start + count + base, length), :] = piece[:, LANES:]
        return square

    square_ref[...] = lax.fori_loop(0, chips // 2, body, jnp.zeros((16, LANES), F32), unroll=32)


def middle(got, t_dev):
    chips = got.shape[0]
    return pl.pallas_call(
        middle_kernel,
        in_specs=[VMEM],
        out_specs=[VMEM] * 2,
        out_shape=[
            pltpu.VMEM((PHASES, chips * t_dev // PHASES, LANES), BF16),
            pltpu.VMEM((16, LANES), F32),
        ],
        scratch_shapes=order_scratch(t_dev),
        compiler_params=SMALL,
    )(local(got))


def spread_kernel(
    got_ref, mine_ref, other_ref, square_ref, days,
    kept_ref, passed_ref, stat_ref,
    edge, line, slid, win, late_win, acc, merged,
):
    chips, rows, _ = got_ref.shape
    count = rows // (PHASES + 1)
    core = lax.rem(lax.axis_index(TM), CORES)
    total_days = 2.0 * chips * count * PHASES
    zero = jnp.zeros((8, LANES), F32)
    sums = mine_ref[chips] + other_ref[chips]
    mean = sums[:, 0:1] / total_days
    var = sums[:, 1:2] / total_days - mean * mean
    row = lax.broadcasted_iota(jnp.int32, (16, LANES), 0)
    column = lax.broadcasted_iota(jnp.int32, (16, LANES), 1) % HALF
    same = (column < USED) & (column % KCOUNT == row)
    mean = jnp.sum(jnp.where(same, mean, 0.0), 0, keepdims=True)
    var = jnp.sum(jnp.where(same, var, 0.0), 0, keepdims=True)
    stat_ref[...] = jnp.concatenate([mean, var, jnp.zeros((6, LANES), F32)], 0)
    lane = lax.broadcasted_iota(jnp.int32, (1, LANES), 1)
    valid = lane % HALF < USED

    def centered(value):
        return jnp.where(valid, (value - mean).astype(BF16).astype(F32), 0.0)

    edge[0] = jnp.broadcast_to(mean, (16, LANES))
    edge[chips + 1] = jnp.broadcast_to(mean, (16, LANES))

    def move(chip, _):
        edge[chip + 1] = other_ref[chip]
        return 0

    lax.fori_loop(0, chips, move, 0, unroll=64)

    def slide(group, sums, target, offset, base):
        sums = list(sums)
        for side in range(8):
            place = 8 * group + side
            chip = chip_at(place)
            at = base + side
            line[at, 0:8, :] = centered(edge[chip + core, 8:16, :])
            line[at, 8 : 8 + count, :] = jnp.where(lane == USED, 1.0, centered(joined(got_ref[place, rows - count :, :])))
            line[at, 8 + count :, :] = centered(edge[chip + core + 1, 0:8, :])
            sums[0] = sums[0] + line[at, 0:16, :] - line[at, count : count + 16, :]
            sums[1] = sums[1] + summed(line[at, 8 : 8 + count, :])
        for side in range(8):
            at = base + side
            slid[at, 0 : count + 15, :] = jnp.where(
                lane < HALF, line[at, 0 : count + 15, :], line[at, 1 : count + 16, :]
            )
        start = (8 * group - offset) * count
        if not isinstance(start, int):
            start = pl.multiple_of(start, 16)
        for pair in range(8 // 2):
            for q in range(TILES):
                tile = jnp.concatenate(
                    [slid[base + 2 * pair + side, 2 * q : 2 * q + count, :] for side in range(2)], 0
                )
                target[q, pl.ds(start + pair * 2 * count, 2 * count), :] = tile.astype(BF16)
        return tuple(sums)

    def multiply(source, rows):
        return lax.dot_general(
            jnp.concatenate([source[q] for q in range(TILES)], 1),
            jnp.concatenate([days[r, rows, :] for r in range(PHASES)], 1),
            (((0,), (0,)), ((), ())),
            preferred_element_type=F32,
        )

    half = chips // 2
    window_sums = lax.fori_loop(
        0, half // 8, lambda g, sums: slide(g, sums, win, 0, 0), (jnp.zeros((16, LANES), F32), zero),
        unroll=True,
    )
    for group in range(half // 8, chips // 8):
        window_sums = slide(group, window_sums, late_win, half, 8 * (group % 2))
    acc[0:WIDTH, :] = multiply(win, slice(0, half * count))
    acc[0:WIDTH, :] += multiply(late_win, slice(half * count, chips * count))
    edges, inner = window_sums
    acc[WIDTH:, :] = jnp.zeros((HALF, PHASES * LANES), F32)
    inner = jnp.sum(inner, 0, keepdims=True)
    at = lax.broadcasted_iota(jnp.int32, (16, LANES), 0)
    upper_half = (lax.broadcasted_iota(jnp.int32, (16, LANES), 1) >= HALF).astype(jnp.int32)
    window_sums = []
    for q in range(TILES):
        move = 2 * q - BEFORE + upper_half
        gained = (at >= 8 + move) & (at < 8)
        lost = (at >= 8) & (at < 8 + move)
        change = jnp.where(gained, edges, 0.0) - jnp.where(lost, edges, 0.0)
        window_sums.append(inner + jnp.sum(change, 0, keepdims=True))
    sums_row = jnp.concatenate(window_sums, 1)

    def shifted(parts):
        total = parts[0]
        lanes = lax.broadcasted_iota(jnp.int32, total.shape, 1) % HALF
        for r in range(1, PHASES):
            near = pltpu.roll(parts[r], WIDTH - KCOUNT * r, 1)
            far = pltpu.roll(parts[r], WIDTH - KCOUNT * r - (HALF - USED), 1)
            total = total + jnp.where(lanes + KCOUNT * r < USED, near, far)
        return total

    squared = jnp.sum(square_ref[...], 0, keepdims=True)
    inside = lax.broadcasted_iota(jnp.int32, (LANES, LANES), 0) % HALF
    for tile in range(TILES):
        base = tile * LANES
        total = acc[base : base + LANES, 0:LANES]
        for r in range(1, PHASES):
            lanes = slice(r * LANES, (r + 1) * LANES)
            near = base + KCOUNT * r
            far = near + HALF - USED
            total = total + jnp.where(
                inside + KCOUNT * r < USED,
                acc[near : near + LANES, lanes],
                acc[far : far + LANES, lanes],
            )
        if base <= SUM_LANE < base + LANES:
            at = lax.broadcasted_iota(jnp.int32, (LANES, LANES), 0) + base
            plain = sum(acc[base : base + LANES, r * LANES : (r + 1) * LANES] for r in range(PHASES))
            total = jnp.where(at == SUM_LANE, plain, total)
            total = jnp.where(at == SQUARE_LANE, squared, total)
        merged[:, base : base + LANES] = jnp.transpose(total)
    totals = shifted([jnp.broadcast_to(sums_row, (8, WIDTH))] * PHASES)
    kept_ref[0:HALF, :] = merged[pl.ds(pl.multiple_of(core * HALF, HALF), HALF), :]
    passed_ref[0:HALF, :] = merged[pl.ds(pl.multiple_of((1 - core) * HALF, HALF), HALF), :]
    for target in (kept_ref, passed_ref):
        target[HALF : HALF + 8, :] = totals
        target[HALF + 8 :, :] = totals


def spread(got, mine, other, square, days):
    chips, rows, _ = got.shape
    count = rows // (PHASES + 1)
    return pl.pallas_call(
        spread_kernel,
        in_specs=[VMEM] * 5,
        out_specs=[VMEM] * 3,
        out_shape=[
            pltpu.VMEM((ROWS, WIDTH), F32),
            pltpu.VMEM((ROWS, WIDTH), F32),
            pltpu.VMEM((8, LANES), F32),
        ],
        scratch_shapes=[
            pltpu.VMEM((chips + 2, 16, LANES), F32),
            pltpu.VMEM((16, count + 16, LANES), F32),
            pltpu.VMEM((16, count + 16, LANES), F32),
            pltpu.VMEM((TILES, chips * count // 2, LANES), BF16),
            pltpu.VMEM((TILES, chips * count // 2, LANES), BF16),
            pltpu.VMEM((WIDTH + HALF, PHASES * LANES), F32),
            pltpu.VMEM((LANES, WIDTH), F32),
        ],
        compiler_params=pltpu.CompilerParams(vmem_limit_bytes=32 << 20),
    )(local(got), local(mine), local(other), local(square), local(days))


def finish_kernel(
    kept_ref, taken_ref, stat_ref, lag_ref, mask_ref, offset_ref, out_ref,
    base, maps, sems, *, total_days,
):
    slots = lax.broadcasted_iota(jnp.int32, (WIDTH + 16, LANES), 0) - 16
    slot = lax.broadcasted_iota(jnp.int32, (1, LANES), 1)
    group = lax.shift_right_logical(slot * 43, 8)
    place = jnp.where(slot < TILES * 2 * PHASES, HALF * group + KCOUNT * (slot - PHASES * group), -100)
    base[...] = (slots == place).astype(F32)
    value = kept_ref[...] + taken_ref[...]
    upper = value.astype(BF16)
    rest = value - upper.astype(F32)
    middle = rest.astype(BF16)
    lower = (rest - middle.astype(F32)).astype(BF16)
    mean_x = value[0:HALF, SUM_LANE : SUM_LANE + 1] / total_days
    var_x = value[0:HALF, SQUARE_LANE : SQUARE_LANE + 1] / total_days - mean_x * mean_x
    scale_x = total_days * jnp.sqrt(var_x + 1e-06)
    scale_i = jnp.sqrt(stat_ref[1:2, :] + 1e-06)
    mask = jnp.concatenate([mask_ref[...].astype(F32), jnp.zeros((1, LANES - HALF), F32)], 1)
    mask = jnp.transpose(jnp.broadcast_to(mask, (LANES, LANES)))[0:HALF, 0:1]
    lags = lag_ref.shape[1]
    lag = jnp.concatenate([lag_ref[...], jnp.zeros((1, LANES - lags), jnp.int32)], 1)
    parts = jnp.concatenate([upper, middle, lower], 0)
    copies = []
    picker = jnp.concatenate([base[16 - k : 16 - k + WIDTH, :].astype(BF16) for k in range(KCOUNT)], 1)
    thirds = jnp.dot(parts, picker, preferred_element_type=F32)
    every = thirds[0:ROWS] + thirds[ROWS : 2 * ROWS] + thirds[2 * ROWS :]
    for pair in range(KCOUNT // 2):
        chosen = every[:, pair * 2 * LANES : (pair + 1) * 2 * LANES]
        for side in range(2):
            k = 2 * pair + side
            part = chosen[:, side * LANES : (side + 1) * LANES]
            wanted = BEFORE * PHASES - (lag + offset_ref[:, k : k + 1])
            part = jnp.take_along_axis(
                part, jnp.broadcast_to(wanted, part.shape), axis=1, mode="promise_in_bounds"
            )
            numer = part[0:HALF] - mean_x * part[HALF : HALF + 1]
            answer = numer / (scale_x * scale_i[:, k : k + 1]) * mask
            maps[k] = answer[:, :lags]
        copy = pltpu.make_async_copy(
            maps.at[2 * pair : 2 * pair + 2], out_ref.at[2 * pair : 2 * pair + 2], sems.at[pair]
        )
        copy.start()
        copies.append(copy)
    for copy in copies:
        copy.wait()


def finish(kept, taken, stat, lag_list, index_offset, mask, total_days):
    lags = lag_list.shape[0]
    return pl.pallas_call(
        lambda *refs: finish_kernel(*refs, total_days=total_days),
        in_specs=[VMEM] * 6,
        out_specs=ANY,
        out_shape=pltpu.HBM((KCOUNT, HALF, lags), F32),
        scratch_shapes=[
            pltpu.VMEM((WIDTH + 16, LANES), F32),
            pltpu.VMEM((KCOUNT, HALF, lags), F32),
            pltpu.SemaphoreType.DMA((KCOUNT // 2,)),
        ],
        compiler_params=SMALL,
    )(
        local(kept), local(taken), local(stat), local(lag_list[None, :]), local(mask[None, :]),
        local(index_offset[None, :]),
    )


def after(got, lag_list, index_offset, sea_mask, total_days, swapped):
    t_dev = got.shape[1] * PHASES // (PHASES + 1)
    mine = take_index(got)
    other = swapped(mine)
    days, square = middle(got, t_dev)
    kept, passed, stat = spread(got, mine, other, square, days)
    taken = swapped(passed)
    maps = finish(kept, taken, stat, lag_list, index_offset, sea_mask, total_days)
    return jnp.transpose(maps, (1, 0, 2))


def shards(field, index, lag_list, index_offset, sea_mask):
    devices = lax.axis_size(TM)
    groups = [
        [CORES * chip_at(place) + core for place in range(devices // CORES)]
        for core in range(CORES)
    ]
    got = lax.all_to_all(
        pack(field, index), TM, 0, 0, axis_index_groups=groups, tiled=True
    )
    total_days = 1.0 * index.shape[0] * devices
    swap = [(i, i ^ 1) for i in range(devices)]
    return after(
        got, lag_list, index_offset, sea_mask, total_days, lambda x: lax.ppermute(x, TM, swap)
    )


def solution(mesh):
    return jax.shard_map(
        shards,
        mesh=mesh,
        in_specs=(P(TM, None), P(TM, None), P(), P(), P(TM)),
        out_specs=P(TM, None, None),
        check_vma=False,
    )
```

```python
import jax
import jax.numpy as jnp
from jax import lax
from jax.experimental import pallas as pl
from jax.experimental.pallas import tpu as pltpu
from jax.sharding import PartitionSpec as P

TM = "tm"
CORES = 2
WEIGHTS = (1, 16, 4)
DIGITS = ((3, 2, 1, 0), (3, 2, 1, 0), (2, 1, 0, 3))
PHASES = 6
KCOUNT = 10
USED = PHASES * KCOUNT
LANES = 128
HALF = 64
BEFORE = 8
TILES = 7
WIDTH = TILES * LANES
SUM_LANE = BEFORE * HALF + USED
SQUARE_LANE = SUM_LANE + 1
ROWS = HALF + 16
STEP = 8
EARLY = 32
F32 = jnp.float32
BF16 = jnp.bfloat16
VMEM = pl.BlockSpec(memory_space=pltpu.VMEM)
ANY = pl.BlockSpec(memory_space=pl.ANY)
SMALL = pltpu.CompilerParams(vmem_limit_bytes=8 << 20)


def chip_at(place):
    chip = 0
    for i, (weight, digits) in enumerate(zip(WEIGHTS, DIGITS)):
        digit = (place >> (4 - 2 * i)) & 3
        table = sum(value << (2 * at) for at, value in enumerate(digits))
        chip = chip + weight * ((table >> (2 * digit)) & 3)
    return chip


def local(array):
    return pltpu.with_memory_space_constraint(array, pltpu.VMEM)


def fill_order(early, late):
    for target in (early, late):
        days = target.shape[0]
        length = days // PHASES
        row = lax.broadcasted_iota(jnp.int32, (length, days), 0)
        column = lax.broadcasted_iota(jnp.int32, (length, days), 1)
        for r in range(PHASES):
            target[r * length : (r + 1) * length, :] = (column == row * PHASES + r).astype(BF16)


def order_scratch(t_dev):
    ahead = EARLY * PHASES
    return [pltpu.VMEM((ahead, ahead), BF16), pltpu.VMEM((t_dev - ahead, t_dev - ahead), BF16)]


def pack_kernel(field_ref, index_ref, sent_ref, index, early, late, sems, index_sem):
    kcount, t_dev = index_ref.shape
    count = t_dev // PHASES
    chips = sent_ref.shape[0]
    ahead = EARLY * PHASES
    index_copy = pltpu.make_async_copy(index_ref, index, index_sem)
    index_copy.start()

    def copy(place):
        lanes = pl.ds(pl.multiple_of(chip_at(place) * LANES, LANES), LANES)
        return pltpu.make_async_copy(
            field_ref.at[:, lanes], sent_ref.at[place, 0:t_dev, :], sems.at[place]
        )

    def start(place, _):
        copy(place).start()
        return 0

    lax.fori_loop(0, chips, start, 0, unroll=8)
    fill_order(early, late)
    index_copy.wait()
    rest = index[...]
    gap = jnp.zeros((16 - kcount, 1), F32)
    rest_sums = jnp.concatenate(
        [
            jnp.sum(rest, 1, keepdims=True),
            gap,
            jnp.sum(rest * rest, 1, keepdims=True),
            jnp.zeros((count - 16 - kcount, 1), F32),
        ],
        0,
    )
    spare = []
    for _ in range(3):
        spare.append(rest_sums.astype(BF16).astype(F32))
        rest_sums = rest_sums - spare[-1]
    spare.append(jnp.zeros((count, 1), F32))
    value = jnp.zeros((count, USED), F32)
    for _ in range(3):
        part = rest.astype(BF16)
        rest = rest - part.astype(F32)
        first = lax.dot_general(
            early[...], part[:, :ahead], (((1,), (1,)), ((), ())), preferred_element_type=F32
        )
        second = lax.dot_general(
            late[...], part[:, ahead:], (((1,), (1,)), ((), ())), preferred_element_type=F32
        )
        later = count - EARLY
        value = value + jnp.concatenate(
            [
                jnp.concatenate(
                    [first[r * EARLY : (r + 1) * EARLY], second[r * later : (r + 1) * later]], 0
                )
                for r in range(PHASES)
            ],
            1,
        )
    origin = value[0:1].astype(BF16).astype(F32)
    top = lax.broadcasted_iota(jnp.int32, value.shape, 0) == 0
    value = jnp.where(top, value, value - origin)
    upper = value.astype(BF16).astype(F32)
    blank = jnp.zeros((count, HALF - USED), F32)
    rows = jnp.concatenate([upper] + spare + [value - upper, blank], 1).astype(BF16)

    def repeat(place, _):
        sent_ref[place, t_dev:, :] = rows
        return 0

    lax.fori_loop(0, chips, repeat, 0, unroll=8)

    def finish_copy(place, _):
        copy(place).wait()
        return 0

    lax.fori_loop(0, chips, finish_copy, 0, unroll=8)


def pack(field, index):
    t_dev, cells = field.shape
    chips = cells // LANES
    return pl.pallas_call(
        pack_kernel,
        in_specs=[ANY] * 2,
        out_specs=VMEM,
        out_shape=pltpu.VMEM((chips, t_dev + t_dev // PHASES, LANES), BF16),
        scratch_shapes=[pltpu.VMEM(index.T.shape, F32)]
        + order_scratch(t_dev)
        + [pltpu.SemaphoreType.DMA((chips,)), pltpu.SemaphoreType.DMA],
        compiler_params=SMALL,
    )(*[pltpu.with_memory_space_constraint(x, pltpu.HBM) for x in (field, index.T)])


def joined(raw):
    wide = raw.astype(F32)
    turned = pltpu.roll(wide, HALF, 1)
    value = wide + turned
    lane = lax.broadcasted_iota(jnp.int32, (1, LANES), 1)
    origin = jnp.where(lane < HALF, wide[0:1], turned[0:1])
    top = lax.broadcasted_iota(jnp.int32, value.shape, 0) == 0
    return jnp.where(top, value, value + origin)


def summed(value):
    return jnp.sum(value.reshape(-1, 8, LANES), 0)


def take_kernel(got_ref, edge_ref):
    chips, rows, _ = got_ref.shape
    count = rows // (PHASES + 1)
    start = rows - count
    lane = lax.broadcasted_iota(jnp.int32, (1, LANES), 1)
    top = lax.broadcasted_iota(jnp.int32, (8, LANES), 0) == 0

    def body(place, sums):
        head = got_ref[place, start : start + 32, :].astype(F32)
        tail = got_ref[place, rows - 8 :, :].astype(F32)
        turned = pltpu.roll(head[0:8], HALF, 1)
        origin = jnp.where(lane < HALF, head[0:1], turned[0:1])
        value = head[0:8] + turned
        chip = chip_at(place)
        edge_ref[chip, 0:8, :] = jnp.where(top, value, value + origin)
        edge_ref[chip, 8:16, :] = tail + pltpu.roll(tail, HALF, 1) + origin
        return sums + head

    sums = lax.fori_loop(0, chips, body, jnp.zeros((32, LANES), F32), unroll=64)
    spare = (lane >= USED) & (lane < HALF)
    sums = jnp.sum(jnp.where(spare, sums, 0.0), 1, keepdims=True)
    edge_ref[chips] = jnp.where(lane == 0, sums[0:16], jnp.where(lane == 1, sums[16:32], 0.0))


def take_index(got):
    return pl.pallas_call(
        take_kernel,
        in_specs=[VMEM],
        out_specs=VMEM,
        out_shape=pltpu.VMEM((got.shape[0] + 1, 16, LANES), F32),
        compiler_params=SMALL,
    )(local(got))


def middle_kernel(got_ref, days_ref, square_ref, early, late):
    chips, rows, _ = got_ref.shape
    t_dev = rows * PHASES // (PHASES + 1)
    count = t_dev // PHASES
    ahead = EARLY * PHASES
    fill_order(early, late)

    def body(pair, square):
        start = pl.multiple_of(pair * 2 * count, 16)
        for source, days, base in ((early, slice(0, ahead), 0), (late, slice(ahead, t_dev), EARLY)):
            length = source.shape[0] // PHASES
            blocks = [got_ref[2 * pair + side, days, :] for side in range(2)]
            for block in blocks:
                wide = block.astype(F32)
                square = square + jnp.sum((wide * wide).reshape(-1, 16, LANES), 0)
            mixed = jnp.dot(
                source[...], jnp.concatenate(blocks, 1), preferred_element_type=F32
            )
            for r in range(PHASES):
                piece = mixed[r * length : (r + 1) * length].astype(BF16)
                days_ref[r, pl.ds(start + base, length), :] = piece[:, :LANES]
                days_ref[r, pl.ds(start + count + base, length), :] = piece[:, LANES:]
        return square

    square_ref[...] = lax.fori_loop(0, chips // 2, body, jnp.zeros((16, LANES), F32), unroll=32)


def middle(got, t_dev):
    chips = got.shape[0]
    return pl.pallas_call(
        middle_kernel,
        in_specs=[VMEM],
        out_specs=[VMEM] * 2,
        out_shape=[
            pltpu.VMEM((PHASES, chips * t_dev // PHASES, LANES), BF16),
            pltpu.VMEM((16, LANES), F32),
        ],
        scratch_shapes=order_scratch(t_dev),
        compiler_params=SMALL,
    )(local(got))


def spread_kernel(
    got_ref, mine_ref, other_ref, square_ref, days,
    kept_ref, passed_ref, stat_ref,
    edge, line, slid, win, late_win, acc, merged,
):
    chips, rows, _ = got_ref.shape
    count = rows // (PHASES + 1)
    core = lax.rem(lax.axis_index(TM), CORES)
    total_days = 2.0 * chips * count * PHASES
    zero = jnp.zeros((8, LANES), F32)
    sums = mine_ref[chips] + other_ref[chips]
    mean = sums[:, 0:1] / total_days
    var = sums[:, 1:2] / total_days - mean * mean
    row = lax.broadcasted_iota(jnp.int32, (16, LANES), 0)
    column = lax.broadcasted_iota(jnp.int32, (16, LANES), 1) % HALF
    same = (column < USED) & (column % KCOUNT == row)
    mean = jnp.sum(jnp.where(same, mean, 0.0), 0, keepdims=True)
    var = jnp.sum(jnp.where(same, var, 0.0), 0, keepdims=True)
    stat_ref[...] = jnp.concatenate([mean, var, jnp.zeros((6, LANES), F32)], 0)
    lane = lax.broadcasted_iota(jnp.int32, (1, LANES), 1)
    valid = lane % HALF < USED

    def centered(value):
        return jnp.where(valid, (value - mean).astype(BF16).astype(F32), 0.0)

    edge[0] = jnp.broadcast_to(mean, (16, LANES))
    edge[chips + 1] = jnp.broadcast_to(mean, (16, LANES))

    def move(chip, _):
        edge[chip + 1] = other_ref[chip]
        return 0

    lax.fori_loop(0, chips, move, 0, unroll=64)

    def slide(group, sums, target, offset, base):
        sums = list(sums)
        for side in range(8):
            place = 8 * group + side
            chip = chip_at(place)
            at = base + side
            line[at, 0:8, :] = centered(edge[chip + core, 8:16, :])
            line[at, 8 : 8 + count, :] = jnp.where(lane == USED, 1.0, centered(joined(got_ref[place, rows - count :, :])))
            line[at, 8 + count :, :] = centered(edge[chip + core + 1, 0:8, :])
            sums[0] = sums[0] + line[at, 0:16, :] - line[at, count : count + 16, :]
            sums[1] = sums[1] + summed(line[at, 8 : 8 + count, :])
        for side in range(8):
            at = base + side
            slid[at, 0 : count + 15, :] = jnp.where(
                lane < HALF, line[at, 0 : count + 15, :], line[at, 1 : count + 16, :]
            )
        start = (8 * group - offset) * count
        if not isinstance(start, int):
            start = pl.multiple_of(start, 16)
        for pair in range(8 // 2):
            for q in range(TILES):
                tile = jnp.concatenate(
                    [slid[base + 2 * pair + side, 2 * q : 2 * q + count, :] for side in range(2)], 0
                )
                target[q, pl.ds(start + pair * 2 * count, 2 * count), :] = tile.astype(BF16)
        return tuple(sums)

    def multiply(source, rows):
        return lax.dot_general(
            jnp.concatenate([source[q] for q in range(TILES)], 1),
            jnp.concatenate([days[r, rows, :] for r in range(PHASES)], 1),
            (((0,), (0,)), ((), ())),
            preferred_element_type=F32,
        )

    half = chips // 2
    window_sums = lax.fori_loop(
        0, half // 8, lambda g, sums: slide(g, sums, win, 0, 0), (jnp.zeros((16, LANES), F32), zero),
        unroll=True,
    )
    for group in range(half // 8, chips // 8):
        window_sums = slide(group, window_sums, late_win, half, 8 * (group % 2))
    acc[0:WIDTH, :] = multiply(win, slice(0, half * count))
    acc[0:WIDTH, :] += multiply(late_win, slice(half * count, chips * count))
    edges, inner = window_sums
    acc[WIDTH:, :] = jnp.zeros((HALF, PHASES * LANES), F32)
    inner = jnp.sum(inner, 0, keepdims=True)
    at = lax.broadcasted_iota(jnp.int32, (16, LANES), 0)
    upper_half = (lax.broadcasted_iota(jnp.int32, (16, LANES), 1) >= HALF).astype(jnp.int32)
    window_sums = []
    for q in range(TILES):
        move = 2 * q - BEFORE + upper_half
        gained = (at >= 8 + move) & (at < 8)
        lost = (at >= 8) & (at < 8 + move)
        change = jnp.where(gained, edges, 0.0) - jnp.where(lost, edges, 0.0)
        window_sums.append(inner + jnp.sum(change, 0, keepdims=True))
    sums_row = jnp.concatenate(window_sums, 1)

    def shifted(parts):
        total = parts[0]
        lanes = lax.broadcasted_iota(jnp.int32, total.shape, 1) % HALF
        for r in range(1, PHASES):
            near = pltpu.roll(parts[r], WIDTH - KCOUNT * r, 1)
            far = pltpu.roll(parts[r], WIDTH - KCOUNT * r - (HALF - USED), 1)
            total = total + jnp.where(lanes + KCOUNT * r < USED, near, far)
        return total

    squared = jnp.sum(square_ref[...], 0, keepdims=True)
    inside = lax.broadcasted_iota(jnp.int32, (LANES, LANES), 0) % HALF
    for tile in range(TILES):
        base = tile * LANES
        total = acc[base : base + LANES, 0:LANES]
        for r in range(1, PHASES):
            lanes = slice(r * LANES, (r + 1) * LANES)
            near = base + KCOUNT * r
            far = near + HALF - USED
            total = total + jnp.where(
                inside + KCOUNT * r < USED,
                acc[near : near + LANES, lanes],
                acc[far : far + LANES, lanes],
            )
        if base <= SUM_LANE < base + LANES:
            at = lax.broadcasted_iota(jnp.int32, (LANES, LANES), 0) + base
            plain = sum(acc[base : base + LANES, r * LANES : (r + 1) * LANES] for r in range(PHASES))
            total = jnp.where(at == SUM_LANE, plain, total)
            total = jnp.where(at == SQUARE_LANE, squared, total)
        merged[:, base : base + LANES] = jnp.transpose(total)
    totals = shifted([jnp.broadcast_to(sums_row, (8, WIDTH))] * PHASES)
    kept_ref[0:HALF, :] = merged[pl.ds(pl.multiple_of(core * HALF, HALF), HALF), :]
    passed_ref[0:HALF, :] = merged[pl.ds(pl.multiple_of((1 - core) * HALF, HALF), HALF), :]
    for target in (kept_ref, passed_ref):
        target[HALF : HALF + 8, :] = totals
        target[HALF + 8 :, :] = totals


def spread(got, mine, other, square, days):
    chips, rows, _ = got.shape
    count = rows // (PHASES + 1)
    return pl.pallas_call(
        spread_kernel,
        in_specs=[VMEM] * 5,
        out_specs=[VMEM] * 3,
        out_shape=[
            pltpu.VMEM((ROWS, WIDTH), F32),
            pltpu.VMEM((ROWS, WIDTH), F32),
            pltpu.VMEM((8, LANES), F32),
        ],
        scratch_shapes=[
            pltpu.VMEM((chips + 2, 16, LANES), F32),
            pltpu.VMEM((16, count + 16, LANES), F32),
            pltpu.VMEM((16, count + 16, LANES), F32),
            pltpu.VMEM((TILES, chips * count // 2, LANES), BF16),
            pltpu.VMEM((TILES, chips * count // 2, LANES), BF16),
            pltpu.VMEM((WIDTH + HALF, PHASES * LANES), F32),
            pltpu.VMEM((LANES, WIDTH), F32),
        ],
        compiler_params=pltpu.CompilerParams(vmem_limit_bytes=32 << 20),
    )(local(got), local(mine), local(other), local(square), local(days))


def finish_kernel(
    kept_ref, taken_ref, stat_ref, lag_ref, mask_ref, offset_ref, out_ref,
    base, maps, sems, *, total_days,
):
    slots = lax.broadcasted_iota(jnp.int32, (WIDTH + 16, LANES), 0) - 16
    slot = lax.broadcasted_iota(jnp.int32, (1, LANES), 1)
    group = lax.shift_right_logical(slot * 43, 8)
    place = jnp.where(slot < TILES * 2 * PHASES, HALF * group + KCOUNT * (slot - PHASES * group), -100)
    base[...] = (slots == place).astype(F32)
    value = kept_ref[...] + taken_ref[...]
    upper = value.astype(BF16)
    rest = value - upper.astype(F32)
    middle = rest.astype(BF16)
    lower = (rest - middle.astype(F32)).astype(BF16)
    mean_x = value[0:HALF, SUM_LANE : SUM_LANE + 1] / total_days
    var_x = value[0:HALF, SQUARE_LANE : SQUARE_LANE + 1] / total_days - mean_x * mean_x
    scale_x = total_days * jnp.sqrt(var_x + 1e-06)
    scale_i = jnp.sqrt(stat_ref[1:2, :] + 1e-06)
    mask = jnp.concatenate([mask_ref[...].astype(F32), jnp.zeros((1, LANES - HALF), F32)], 1)
    mask = jnp.transpose(jnp.broadcast_to(mask, (LANES, LANES)))[0:HALF, 0:1]
    lags = lag_ref.shape[1]
    lag = jnp.concatenate([lag_ref[...], jnp.zeros((1, LANES - lags), jnp.int32)], 1)
    parts = jnp.concatenate([upper, middle, lower], 0)
    copies = []
    for pair in range(KCOUNT // 2):
        picker = jnp.concatenate(
            [base[16 - k : 16 - k + WIDTH, :].astype(BF16) for k in (2 * pair, 2 * pair + 1)], 1
        )
        thirds = jnp.dot(parts, picker, preferred_element_type=F32)
        chosen = thirds[0:ROWS] + thirds[ROWS : 2 * ROWS] + thirds[2 * ROWS :]
        for side in range(2):
            k = 2 * pair + side
            part = chosen[:, side * LANES : (side + 1) * LANES]
            wanted = BEFORE * PHASES - (lag + offset_ref[:, k : k + 1])
            part = jnp.take_along_axis(
                part, jnp.broadcast_to(wanted, part.shape), axis=1, mode="promise_in_bounds"
            )
            numer = part[0:HALF] - mean_x * part[HALF : HALF + 1]
            answer = numer / (scale_x * scale_i[:, k : k + 1]) * mask
            maps[k] = answer[:, :lags]
        copy = pltpu.make_async_copy(
            maps.at[2 * pair : 2 * pair + 2], out_ref.at[2 * pair : 2 * pair + 2], sems.at[pair]
        )
        copy.start()
        copies.append(copy)
    for copy in copies:
        copy.wait()


def finish(kept, taken, stat, lag_list, index_offset, mask, total_days):
    lags = lag_list.shape[0]
    return pl.pallas_call(
        lambda *refs: finish_kernel(*refs, total_days=total_days),
        in_specs=[VMEM] * 6,
        out_specs=ANY,
        out_shape=pltpu.HBM((KCOUNT, HALF, lags), F32),
        scratch_shapes=[
            pltpu.VMEM((WIDTH + 16, LANES), F32),
            pltpu.VMEM((KCOUNT, HALF, lags), F32),
            pltpu.SemaphoreType.DMA((KCOUNT // 2,)),
        ],
        compiler_params=SMALL,
    )(
        local(kept), local(taken), local(stat), local(lag_list[None, :]), local(mask[None, :]),
        local(index_offset[None, :]),
    )


def after(got, lag_list, index_offset, sea_mask, total_days, swapped):
    t_dev = got.shape[1] * PHASES // (PHASES + 1)
    mine = take_index(got)
    other = swapped(mine)
    days, square = middle(got, t_dev)
    kept, passed, stat = spread(got, mine, other, square, days)
    taken = swapped(passed)
    maps = finish(kept, taken, stat, lag_list, index_offset, sea_mask, total_days)
    return jnp.transpose(maps, (1, 0, 2))


def shards(field, index, lag_list, index_offset, sea_mask):
    devices = lax.axis_size(TM)
    groups = [
        [CORES * chip_at(place) + core for place in range(devices // CORES)]
        for core in range(CORES)
    ]
    got = lax.all_to_all(
        pack(field, index), TM, 0, 0, axis_index_groups=groups, tiled=True
    )
    total_days = 1.0 * index.shape[0] * devices
    swap = [(i, i ^ 1) for i in range(devices)]
    return after(
        got, lag_list, index_offset, sea_mask, total_days, lambda x: lax.ppermute(x, TM, swap)
    )


def solution(mesh):
    return jax.shard_map(
        shards,
        mesh=mesh,
        in_specs=(P(TM, None), P(TM, None), P(), P(), P(TM)),
        out_specs=P(TM, None, None),
        check_vma=False,
    )
```
